8 devices in a mesh: dp: 1 (over z), tp: 8 (over x, y, core).
Axes of the slice: x: 2, y: 2, z: 1, core: 2. Of those that a mesh axis runs over, the one named last changes fastest.
Arguments:
- x: bfloat16 [64, 3072], P('dp')
- k_cache: bfloat16 [64, 4096, 8, 128], P('dp', None, 'tp')
- v_cache: bfloat16 [64, 4096, 8, 128], P('dp', None, 'tp')
- gain_a: bfloat16 [3072], replicated
- wq: bfloat16 [3072, 3072], P(None, 'tp')
- wo: bfloat16 [3072, 3072], P('tp')
- gain_m: bfloat16 [3072], replicated
- w_gate: bfloat16 [3072, 8192], P(None, 'tp')
- w_up: bfloat16 [3072, 8192], P(None, 'tp')
- w_down: bfloat16 [8192, 3072], P('tp')
Outputs:
- output: bfloat16 [64, 3072], P('dp')
All inputs are finite; a program needn't handle non-finite values.
Results may differ from the reference program's by a relative error of at most 0.017.
Values are sent between devices in bfloat16 or wider.
A program may use at most 2 GiB of HBM per device.

```python
import jax
import jax.numpy as jnp
from jax import lax

BATCH = 64
CACHE = 4096
D = 3072
HEADS = 24
KV_HEADS = 8
HEAD = 128
FF = 8192
THETA = 10000


def setup_inputs(seed: int = 0, part: int = 0) -> dict:
    kx, kc, kw, kn, kq, ko, km, kg, ku, kd = jax.random.split(jax.random.key(seed), 10)
    kx, kc, kw = (jax.random.fold_in(k, part) for k in (kx, kc, kw))

    def weights(key, rows, columns):
        return jax.random.normal(key, (rows, columns), jnp.float32) * rows**-0.5

    drawn = {
        "x": jax.random.normal(kx, (BATCH, D), jnp.float32),
        "k_cache": 2 * jax.random.normal(kc, (BATCH, CACHE, KV_HEADS, HEAD), jnp.float32),
        "v_cache": 4 * jax.random.normal(kw, (BATCH, CACHE, KV_HEADS, HEAD), jnp.float32),
        "gain_a": 1 + 0.1 * jax.random.normal(kn, (D,), jnp.float32),
        "wq": 2 * weights(kq, D, HEADS * HEAD),
        "wo": weights(ko, HEADS * HEAD, D),
        "gain_m": 1 + 0.1 * jax.random.normal(km, (D,), jnp.float32),
        "w_gate": weights(kg, D, FF),
        "w_up": weights(ku, D, FF),
        "w_down": 2 * weights(kd, FF, D),
    }
    return {k: v.astype(jnp.bfloat16) for k, v in drawn.items()}


def normed(x, gain):
    wide = x.astype(jnp.float32)
    scale = lax.rsqrt(jnp.mean(wide * wide, -1, keepdims=True) + 1e-6)
    return (wide * scale * gain.astype(jnp.float32)).astype(jnp.bfloat16)


def turned(t, place, theta):
    half = t.shape[-1] // 2
    angle = place.astype(jnp.float32)[:, None] * theta ** (-jnp.arange(half, dtype=jnp.float32) / half)
    cos, sin = jnp.cos(angle)[:, None], jnp.sin(angle)[:, None]
    a, b = t[..., :half].astype(jnp.float32), t[..., half:].astype(jnp.float32)
    return jnp.concatenate([a * cos - b * sin, b * cos + a * sin], -1).astype(jnp.bfloat16)


def matmul(a, w):
    return jnp.dot(a, w, preferred_element_type=jnp.float32).astype(jnp.bfloat16)


def einsum(form, a, b):
    return jnp.einsum(form, a.astype(jnp.float32), b.astype(jnp.float32))


def seen_by(a, wq, k_cache, v_cache, head, theta):
    batch, cache, kv_heads = k_cache.shape[:3]
    place = jnp.full((batch,), cache - 1)
    q = turned(matmul(a, wq).reshape(batch, -1, head), place, theta).reshape(batch, kv_heads, -1, head)
    scores = einsum("bgsd,bugd->bgsu", q, k_cache) * head**-0.5
    weights = jax.nn.softmax(scores, -1).astype(jnp.bfloat16)
    return einsum("bgsu,bugd->bgsd", weights, v_cache).astype(jnp.bfloat16).reshape(batch, -1)


def hidden_of(b, w_gate, w_up):
    gate = jnp.dot(b, w_gate, preferred_element_type=jnp.float32)
    up = jnp.dot(b, w_up, preferred_element_type=jnp.float32)
    return (jax.nn.silu(gate) * up).astype(jnp.bfloat16)


def reference(x, k_cache, v_cache, gain_a, wq, wo, gain_m, w_gate, w_up, w_down):
    seen = seen_by(normed(x, gain_a), wq, k_cache, v_cache, HEAD, THETA)
    h = (x.astype(jnp.float32) + jnp.dot(seen, wo, preferred_element_type=jnp.float32)).astype(jnp.bfloat16)
    hidden = hidden_of(normed(h, gain_m), w_gate, w_up)
    return (h.astype(jnp.float32) + jnp.dot(hidden, w_down, preferred_element_type=jnp.float32)).astype(jnp.bfloat16)
```

```python
import functools, math
import jax, jax.numpy as jnp, numpy as np
from jax import lax
from jax.experimental import pallas as pl
from jax.experimental.pallas import tpu as pltpu
from jax.sharding import PartitionSpec as P

HEAD=128; THETA=10000; D=3072; B=64; U=4096; Q=4; G=B//Q; NS=3; UC=512
ANY=pl.BlockSpec(memory_space=pl.ANY); VM=pl.BlockSpec(memory_space=pltpu.VMEM)

def normed(x, gain):
    w = x.astype(jnp.float32)
    s = lax.rsqrt(jnp.mean(w*w, -1, keepdims=True)+1e-6)
    return (w*s*gain.astype(jnp.float32)).astype(jnp.bfloat16)

def rot_tables():
    half=HEAD//2
    ang=(U-1)*THETA**(-np.arange(half,dtype=np.float64)/half)
    c,s=np.cos(ang),np.sin(ang)
    return np.concatenate([c,c])[None].astype(np.float32), np.concatenate([-s,s])[None].astype(np.float32)

def att_kernel(x_ref, ga_ref, cos_ref, sin_ref, wq_hbm, wo_hbm, k_hbm, v_hbm, out_ref,
               kbuf, vbuf, wq, wo, qblk, sbuf, oall, ksem, vsem, wsem):
    def kcopy(g, slot):
        return pltpu.make_async_copy(k_hbm.at[pl.ds(g*Q,Q)], kbuf.at[slot], ksem.at[slot])
    def vcopy(g, slot):
        return pltpu.make_async_copy(v_hbm.at[pl.ds(g*Q,Q)], vbuf.at[slot], vsem.at[slot])
    wqc=pltpu.make_async_copy(wq_hbm, wq, wsem.at[0]); wqc.start()
    kcopy(0,0).start(); kcopy(1,1).start(); vcopy(0,0).start(); kcopy(2,2).start(); vcopy(1,1).start()
    woc=pltpu.make_async_copy(wo_hbm, wo, wsem.at[1]); woc.start()
    a = normed(x_ref[...], ga_ref[...])
    wqc.wait()
    q = jnp.dot(a, wq[...], preferred_element_type=jnp.float32).astype(jnp.bfloat16).astype(jnp.float32)
    C, S = cos_ref[...], sin_ref[...]
    r = lax.broadcasted_iota(jnp.int32,(16*G,B),0); s = lax.broadcasted_iota(jnp.int32,(16*G,B),1)
    rr, gg = r%16, r//16
    qa = jnp.zeros((16*G,HEAD),jnp.float32)
    for h in range(3):
        qh=q[:,h*HEAD:(h+1)*HEAD]
        t=(qh*C+pltpu.roll(qh,HEAD//2,1)*S).astype(jnp.bfloat16)
        E=((s==gg*Q+rr-h*Q)&(rr>=h*Q)&(rr<(h+1)*Q)).astype(jnp.bfloat16)
        qa += jnp.dot(E,t,preferred_element_type=jnp.float32)
    rowl=lax.broadcasted_iota(jnp.int32,(16*G,HEAD),0)%Q
    for sl in range(Q):
        qblk[:,sl*HEAD:(sl+1)*HEAD]=jnp.where(rowl==sl,qa,0.).astype(jnp.bfloat16)
    rowo=lax.broadcasted_iota(jnp.int32,(16,HEAD),0)%Q

    def scores(g, kslot, sslot):
        ql=qblk[pl.ds(pl.multiple_of(g*16,16),16),:]
        for c in range(U//UC):
            kc=jnp.concatenate([kbuf[kslot,i,c*UC:(c+1)*UC,:] for i in range(Q)],axis=1)
            sbuf[sslot,:,c*UC:(c+1)*UC]=lax.dot_general(ql,kc,(((1,),(1,)),((),())),preferred_element_type=jnp.float32)
    def attend(g, vslot, sslot):
        sc=sbuf[sslot]
        m=jnp.max(sc,axis=1,keepdims=True)
        p=jnp.exp2((sc-m)*(HEAD**-0.5*math.log2(math.e)))
        l=jnp.sum(p,axis=1,keepdims=True)
        w=(p*(1.0/l)).astype(jnp.bfloat16)
        o=jnp.zeros((16,Q*HEAD),jnp.float32)
        for c in range(U//UC):
            vc=jnp.concatenate([vbuf[vslot,i,c*UC:(c+1)*UC,:] for i in range(Q)],axis=1)
            o=o+jnp.dot(w[:,c*UC:(c+1)*UC],vc,preferred_element_type=jnp.float32)
        t=jnp.zeros((16,HEAD),jnp.float32)
        for i in range(Q):
            t=jnp.where(rowo==i,o[:,i*HEAD:(i+1)*HEAD],t)
        oall[pl.ds(pl.multiple_of(g*16,16),16),:]=t.astype(jnp.bfloat16)

    kcopy(0,0).wait()
    scores(0,0,0)
    def body(g, _):
        kn=lax.rem(g+1,NS); vn=lax.rem(g,NS)
        kcopy(g+1,kn).wait(); vcopy(g,vn).wait()
        @pl.when(g+3<G)
        def _(): kcopy(g+3,vn).start()
        @pl.when(g+2<G)
        def _(): vcopy(g+2,lax.rem(g+2,NS)).start()
        scores(g+1,kn,lax.rem(g+1,2))
        attend(g,vn,lax.rem(g,2))
        return 0
    lax.fori_loop(0,G-1,body,0)
    vcopy(G-1,(G-1)%NS).wait()
    attend(G-1,(G-1)%NS,(G-1)%2)
    woc.wait()
    rT = lax.broadcasted_iota(jnp.int32,(B,16*G),1); sT = lax.broadcasted_iota(jnp.int32,(B,16*G),0)
    rr, gg = rT%16, rT//16
    acc=jnp.zeros((B,D),jnp.float32)
    seen=[]
    for h in range(3):
        E=((sT==gg*Q+rr-h*Q)&(rr>=h*Q)&(rr<(h+1)*Q)).astype(jnp.bfloat16)
        seen.append(jnp.dot(E,oall[...],preferred_element_type=jnp.float32).astype(jnp.bfloat16))
    out_ref[...]=jnp.dot(jnp.concatenate(seen,axis=1),wo[...],preferred_element_type=jnp.float32).astype(jnp.bfloat16)

def attention_partial(x, k, v, ga, wq, wo):
    C,S=rot_tables()
    return pl.pallas_call(att_kernel,
        out_shape=jax.ShapeDtypeStruct((B,D),jnp.bfloat16),
        in_specs=[VM,VM,VM,VM,ANY,ANY,ANY,ANY], out_specs=VM,
        scratch_shapes=[pltpu.VMEM((NS,Q,U,HEAD),jnp.bfloat16),pltpu.VMEM((NS,Q,U,HEAD),jnp.bfloat16),
            pltpu.VMEM((D,384),jnp.bfloat16),pltpu.VMEM((384,D),jnp.bfloat16),pltpu.VMEM((16*G,Q*HEAD),jnp.bfloat16),
            pltpu.VMEM((2,16,U),jnp.float32),pltpu.VMEM((16*G,HEAD),jnp.bfloat16),
            pltpu.SemaphoreType.DMA((NS,)),pltpu.SemaphoreType.DMA((NS,)),pltpu.SemaphoreType.DMA((2,))],
        compiler_params=pltpu.CompilerParams(vmem_limit_bytes=60*2**20),
        name="att",
    )(x,ga[None],jnp.asarray(C),jnp.asarray(S),wq,wo,k.reshape(B,U,HEAD),v.reshape(B,U,HEAD))

def hidden_of(b, w_gate, w_up):
    gate = jnp.dot(b, w_gate, preferred_element_type=jnp.float32)
    up = jnp.dot(b, w_up, preferred_element_type=jnp.float32)
    return (jax.nn.silu(gate) * up).astype(jnp.bfloat16)

def solution(mesh):
    def added(t, term):
        return (t.astype(jnp.float32) + lax.psum(term.astype(jnp.bfloat16), "tp").astype(jnp.float32)).astype(jnp.bfloat16)
    def step(x, k_cache, v_cache, gain_a, wq, wo, gain_m, w_gate, w_up, w_down):
        h = added(x, attention_partial(x,k_cache,v_cache,gain_a,wq,wo))
        return added(h, jnp.dot(hidden_of(normed(h, gain_m), w_gate, w_up), w_down, preferred_element_type=jnp.float32))
    states, cache, columns, rows_of = P("dp", None), P("dp", None, "tp", None), P(None, "tp"), P("tp", None)
    return jax.shard_map(step, mesh=mesh,
        in_specs=(states, cache, cache, P(None), columns, rows_of, P(None), columns, columns, rows_of),
        out_specs=states, check_vma=False)
```

```python
import math

import jax
import jax.numpy as jnp
import numpy as np
from jax import lax
from jax.experimental import pallas as pl
from jax.experimental.pallas import tpu as pltpu
from jax.sharding import PartitionSpec as P

HEAD = 128
THETA = 10000
D = 3072
B = 64
U = 4096
Q = 4
G = B // Q
NS = 3
UC = 512
N = 8
W = D // N
HID = 1024
CHUNKS = ((0, 12), (12, 4))
REDUCE_AT = 13
QUERIES = 3
F32, BF16 = jnp.float32, jnp.bfloat16
MESH = pl.DeviceIdType.MESH


def rotary_tables():
    half = HEAD // 2
    angle = (U - 1) * THETA ** (-np.arange(half, dtype=np.float64) / half)
    cos, sin = np.cos(angle), np.sin(angle)
    return np.concatenate([cos, cos])[None].astype(np.float32), np.concatenate([-sin, sin])[None].astype(np.float32)


def row(gain):
    return jnp.concatenate([gain[i : i + 1] for i in range(gain.shape[0])], axis=1)


def dot(a, b):
    return jnp.dot(a, b, preferred_element_type=F32)


def layer(x_ref, ga_ref, gm_ref, cos_ref, sin_ref, wq_hbm, wo_hbm, wg_hbm, wu_hbm, wd_hbm, k_hbm, v_hbm, out_ref,
          kbuf, vbuf, wq, wo, wg, wu, wd, qblk, sbuf, oall, bbuf, hid, *rest):
    nc = len(CHUNKS)
    own, part1, part2, recv1, recv2, hbuf, ybuf = (rest[i * nc : (i + 1) * nc] for i in range(7))
    ksem, vsem, wsem, send_sem, recv_sem = rest[7 * nc :]
    me = lax.axis_index("tp")

    def at(d):
        return lax.rem(me + d, N)

    barrier = pltpu.get_barrier_semaphore()
    for d in range(1, N):
        pl.semaphore_signal(barrier, inc=1, device_id={"tp": at(d)}, device_id_type=MESH)

    def kcopy(g, slot):
        return pltpu.make_async_copy(k_hbm.at[pl.ds(g * Q, Q)], kbuf.at[slot], ksem.at[slot])

    def vcopy(g, slot):
        return pltpu.make_async_copy(v_hbm.at[pl.ds(g * Q, Q)], vbuf.at[slot], vsem.at[slot])

    half = HID // 2
    loads = {"wq": pltpu.make_async_copy(wq_hbm, wq, wsem.at[0]), "wo": pltpu.make_async_copy(wo_hbm, wo, wsem.at[1])}
    for n in range(2):
        cols = pl.ds(n * half, half)
        loads["wg", n] = pltpu.make_async_copy(wg_hbm.at[:, cols], wg.at[:, cols], wsem.at[2 + n])
        loads["wu", n] = pltpu.make_async_copy(wu_hbm.at[:, cols], wu.at[:, cols], wsem.at[4 + n])
    loads["wd"] = pltpu.make_async_copy(wd_hbm, wd, wsem.at[6])

    def scatter(c, stage, src, dst):
        return [pltpu.make_async_remote_copy(src.at[at(d)], dst.at[d], send_sem.at[c, stage, d], recv_sem.at[c, stage, d],
                                             device_id={"tp": at(d)}, device_id_type=MESH) for d in range(1, N)]

    def gather(c, stage, buf):
        return [pltpu.make_async_remote_copy(buf.at[me], buf.at[me], send_sem.at[c, stage, d], recv_sem.at[c, stage, d],
                                             device_id={"tp": at(d)}, device_id_type=MESH) for d in range(1, N)]

    def start(copies):
        for copy in copies:
            copy.start()

    def arrived(copies):
        for copy in copies:
            copy.wait_recv()

    def rows_of(c):
        return CHUNKS[c][0] * Q, CHUNKS[c][1] * Q

    loads["wq"].start()
    kcopy(0, 0).start()
    kcopy(1, 1).start()
    vcopy(0, 0).start()
    kcopy(2, 2).start()
    vcopy(1, 1).start()
    loads["wo"].start()
    wide = x_ref[...].astype(F32)
    scale = lax.rsqrt(jnp.mean(wide * wide, -1, keepdims=True) + 1e-6)
    a = (wide * scale * row(ga_ref[...].astype(F32))).astype(BF16)
    loads["wq"].wait()
    q = dot(a, wq[...]).astype(BF16).astype(F32)

    def picks(shape, row_axis, first):
        r = lax.broadcasted_iota(jnp.int32, shape, row_axis)
        s = lax.broadcasted_iota(jnp.int32, shape, 1 - row_axis) + first * Q
        rr = r % 16
        gg = r // 16 + first
        return [((s == gg * Q + rr - h * Q) & (rr >= h * Q) & (rr < (h + 1) * Q)).astype(BF16) for h in range(QUERIES)]

    qa = jnp.zeros((16 * G, HEAD), F32)
    for h, pick in enumerate(picks((16 * G, B), 0, 0)):
        qh = q[:, h * HEAD : (h + 1) * HEAD]
        qa += dot(pick, (qh * cos_ref[...] + pltpu.roll(qh, HEAD // 2, 1) * sin_ref[...]).astype(BF16))
    block = lax.broadcasted_iota(jnp.int32, (16 * G, HEAD), 0) % Q
    for i in range(Q):
        qblk[:, i * HEAD : (i + 1) * HEAD] = jnp.where(block == i, qa, 0.0).astype(BF16)
    block = lax.broadcasted_iota(jnp.int32, (16, HEAD), 0) % Q

    def quad_rows(g):
        return pl.ds(pl.multiple_of(g * 16, 16), 16)

    def scores(g, slot, to):
        ql = qblk[quad_rows(g), :]
        for u in range(0, U, UC):
            kc = jnp.concatenate([kbuf[slot, i, u : u + UC, :] for i in range(Q)], axis=1)
            sbuf[to, :, u : u + UC] = lax.dot_general(ql, kc, (((1,), (1,)), ((), ())), preferred_element_type=F32)

    def attend(g, slot, of):
        s = sbuf[of]
        p = jnp.exp2((s - jnp.max(s, axis=1, keepdims=True)) * (HEAD**-0.5 * math.log2(math.e)))
        w = (p * (1.0 / jnp.sum(p, axis=1, keepdims=True))).astype(BF16)
        o = jnp.zeros((16, Q * HEAD), F32)
        for u in range(0, U, UC):
            o += dot(w[:, u : u + UC], jnp.concatenate([vbuf[slot, i, u : u + UC, :] for i in range(Q)], axis=1))
        t = jnp.zeros((16, HEAD), F32)
        for i in range(Q):
            t = jnp.where(block == i, o[:, i * HEAD : (i + 1) * HEAD], t)
        oall[quad_rows(g), :] = t.astype(BF16)

    def terms(c, a, w_ref, part):
        for n in range(4):
            t = dot(a, w_ref[:, n * 2 * W : (n + 1) * 2 * W])
            for j in range(2):
                own[c][2 * n + j] = t[:, j * W : (j + 1) * W]
                part[2 * n + j] = t[:, j * W : (j + 1) * W].astype(BF16)

    def finish(c):
        first, quads = CHUNKS[c]
        o = oall[first * 16 : (first + quads) * 16, :]
        seen = [dot(pick, o).astype(BF16) for pick in picks((quads * Q, quads * 16), 1, first)]
        if c == 0:
            loads["wo"].wait()
            pl.semaphore_wait(barrier, N - 1)
        terms(c, jnp.concatenate(seen, axis=1), wo, part1[c])
        start(scatter(c, 0, part1[c], recv1[c]))

    def summed(c, stage, part, recv):
        arrived(scatter(c, stage, part, recv))
        t = own[c][me]
        for d in range(1, N):
            t += recv[d].astype(F32)
        return t

    def reduce1(c):
        first, rows = rows_of(c)
        t = summed(c, 0, part1[c], recv1[c])
        mine = x_ref[first : first + rows, pl.ds(pl.multiple_of(me * W, 128), W)].astype(F32)
        hbuf[c][me] = (mine + t).astype(BF16)
        start(gather(c, 1, hbuf[c]))

    def reduce2(c):
        t = summed(c, 2, part2[c], recv2[c])
        ybuf[c][me] = (hbuf[c][me].astype(F32) + t).astype(BF16)
        start(gather(c, 3, ybuf[c]))

    def norm2(c):
        first, rows = rows_of(c)
        arrived(gather(c, 1, hbuf[c]))
        squares = jnp.zeros((rows, 1), F32)
        for j in range(N):
            t = hbuf[c][j].astype(F32)
            squares += jnp.sum(t * t, -1, keepdims=True)
        scale = lax.rsqrt(squares * (1.0 / D) + 1e-6)
        gain = row(gm_ref[...].astype(F32))
        for j in range(N):
            bbuf[first : first + rows, j * W : (j + 1) * W] = (hbuf[c][j].astype(F32) * scale * gain[:, j * W : (j + 1) * W]).astype(BF16)

    def hidden(c, n):
        first, rows = rows_of(c)
        if c == 0:
            loads["wg", n].wait()
            loads["wu", n].wait()
        b = bbuf[first : first + rows, :]
        gate = dot(b, wg[:, n * half : (n + 1) * half])
        up = dot(b, wu[:, n * half : (n + 1) * half])
        hid[first : first + rows, n * half : (n + 1) * half] = (jax.nn.silu(gate) * up).astype(BF16)

    def down(c):
        first, rows = rows_of(c)
        if c == 0:
            loads["wd"].wait()
        terms(c, hid[first : first + rows, :], wd, part2[c])
        start(scatter(c, 2, part2[c], recv2[c]))

    kcopy(0, 0).wait()
    scores(0, 0, 0)

    def body(g, _):
        kslot, vslot = lax.rem(g + 1, NS), lax.rem(g, NS)
        kcopy(g + 1, kslot).wait()
        vcopy(g, vslot).wait()

        @pl.when(g + 3 < G)
        def _():
            kcopy(g + 3, vslot).start()

        @pl.when(g + 2 < G)
        def _():
            vcopy(g + 2, lax.rem(g + 2, NS)).start()

        scores(g + 1, kslot, lax.rem(g + 1, 2))
        attend(g, vslot, lax.rem(g, 2))

        @pl.when(g == CHUNKS[0][1] - 1)
        def _():
            finish(0)

        @pl.when(g == REDUCE_AT)
        def _():
            reduce1(0)

        return 0

    lax.fori_loop(0, G - 1, body, 0)
    vcopy(G - 1, (G - 1) % NS).wait()
    for n in range(2):
        loads["wg", n].start()
        loads["wu", n].start()
    loads["wd"].start()
    attend(G - 1, (G - 1) % NS, (G - 1) % 2)
    finish(1)
    norm2(0)
    hidden(0, 0)
    reduce1(1)
    hidden(0, 1)
    down(0)
    norm2(1)
    hidden(1, 0)
    hidden(1, 1)
    down(1)
    reduce2(0)
    reduce2(1)
    for c in range(nc):
        first, rows = rows_of(c)
        arrived(gather(c, 3, ybuf[c]))
        for j in range(N):
            out_ref[first : first + rows, j * W : (j + 1) * W] = ybuf[c][j]
    for c in range(nc):
        for copies in (scatter(c, 0, part1[c], recv1[c]), gather(c, 1, hbuf[c]), scatter(c, 2, part2[c], recv2[c]), gather(c, 3, ybuf[c])):
            for copy in copies:
                copy.wait_send()


def solution(mesh):
    any_, vmem = pl.BlockSpec(memory_space=pl.ANY), pl.BlockSpec(memory_space=pltpu.VMEM)

    def step(x, k_cache, v_cache, gain_a, wq, wo, gain_m, w_gate, w_up, w_down):
        cos, sin = rotary_tables()

        def blocks(dtype, lead=N):
            return [pltpu.VMEM((lead, quads * Q, W), dtype) for _, quads in CHUNKS]

        nc = len(CHUNKS)
        return pl.pallas_call(
            layer,
            out_shape=jax.ShapeDtypeStruct((B, D), BF16),
            in_specs=[vmem] * 5 + [any_] * 7,
            out_specs=vmem,
            scratch_shapes=[
                pltpu.VMEM((NS, Q, U, HEAD), BF16),
                pltpu.VMEM((NS, Q, U, HEAD), BF16),
                pltpu.VMEM((D, QUERIES * HEAD), BF16),
                pltpu.VMEM((QUERIES * HEAD, D), BF16),
                pltpu.VMEM((D, HID), BF16),
                pltpu.VMEM((D, HID), BF16),
                pltpu.VMEM((HID, D), BF16),
                pltpu.VMEM((16 * G, Q * HEAD), BF16),
                pltpu.VMEM((2, 16, U), F32),
                pltpu.VMEM((16 * G, HEAD), BF16),
                pltpu.VMEM((B, D), BF16),
                pltpu.VMEM((B, HID), BF16),
                *blocks(F32), *blocks(BF16), *blocks(BF16), *blocks(BF16), *blocks(BF16), *blocks(BF16), *blocks(BF16),
                pltpu.SemaphoreType.DMA((NS,)),
                pltpu.SemaphoreType.DMA((NS,)),
                pltpu.SemaphoreType.DMA((7,)),
                pltpu.SemaphoreType.DMA((nc, 4, N)),
                pltpu.SemaphoreType.DMA((nc, 4, N)),
            ],
            compiler_params=pltpu.CompilerParams(collective_id=0, has_side_effects=True, vmem_limit_bytes=62 * 2**20),
            name="layer",
        )(x, gain_a.reshape(-1, 128), gain_m.reshape(-1, 128), jnp.asarray(cos), jnp.asarray(sin), wq, wo, w_gate, w_up, w_down,
          k_cache.reshape(B, U, HEAD), v_cache.reshape(B, U, HEAD))

    states, cache, columns, rows_of = P("dp", None), P("dp", None, "tp", None), P(None, "tp"), P("tp", None)
    return jax.shard_map(
        step,
        mesh=mesh,
        in_specs=(states, cache, cache, P(None), columns, rows_of, P(None), columns, columns, rows_of),
        out_specs=states,
        check_vma=False,
    )
```

```python
import math

import jax
import jax.numpy as jnp
import numpy as np
from jax import lax
from jax.experimental import pallas as pl
from jax.experimental.pallas import tpu as pltpu
from jax.sharding import PartitionSpec as P

HEAD = 128
THETA = 10000
D = 3072
B = 64
U = 4096
Q = 4
G = B // Q
NS = 3
UC = 512
ULAST = 1024
N = 8
W = D // N
HID = 1024
PARTS = ((0, 8, 9), (8, 4, 13), (12, 4, None))
GROUPS = ((0, 48), (48, 16))
QUERIES = 3
F32, BF16 = jnp.float32, jnp.bfloat16
MESH = pl.DeviceIdType.MESH


def rotary_tables():
    half = HEAD // 2
    angle = (U - 1) * THETA ** (-np.arange(half, dtype=np.float64) / half)
    cos, sin = np.cos(angle), np.sin(angle)
    return np.stack([np.concatenate([cos, cos]), np.concatenate([-sin, sin])]).astype(np.float32)


def row(gain):
    return jnp.concatenate([gain[i : i + 1] for i in range(gain.shape[0])], axis=1)


def dot(a, b):
    return jnp.dot(a, b, preferred_element_type=F32)


def layer(x_hbm, ga_hbm, gm_hbm, turn_hbm, wq_hbm, wo_hbm, wg_hbm, wu_hbm, wd_hbm, k_hbm, v_hbm, out_ref,
          x_ref, ga_ref, gm_ref, turn_ref, kbuf, vbuf, wq, wo, wg, wu, wd, qblk, sbuf, wbuf, oall, bbuf, hid, own, part1, part2, recv1, recv2, hbuf, ybuf,
          ksem, vsem, lastsem, wsem, send_sem, recv_sem):
    me = lax.axis_index("tp")
    mx, my, mc = me // 4, lax.rem(me // 2, 2), lax.rem(me, 2)

    def chip(k):
        return 2 * lax.rem(mx + k // 2, 2) + lax.rem(my + k % 2, 2)

    def at(s):
        return 2 * chip(s // 2) + lax.rem(mc + s % 2, 2)

    def kcopy(g, slot):
        return pltpu.make_async_copy(k_hbm.at[pl.ds(g * Q, Q)], kbuf.at[slot], ksem.at[slot])

    def vcopy(g, slot):
        return pltpu.make_async_copy(v_hbm.at[pl.ds(g * Q, Q)], vbuf.at[slot], vsem.at[slot])

    half = HID // 2
    loads = {"wq": pltpu.make_async_copy(wq_hbm, wq, wsem.at[0]), "wo": pltpu.make_async_copy(wo_hbm, wo, wsem.at[1])}
    for n in range(2):
        cols = pl.ds(n * half, half)
        loads["wg", n] = pltpu.make_async_copy(wg_hbm.at[:, cols], wg.at[:, cols], wsem.at[2 + n])
        loads["wu", n] = pltpu.make_async_copy(wu_hbm.at[:, cols], wu.at[:, cols], wsem.at[4 + n])
    loads["wd"] = pltpu.make_async_copy(wd_hbm, wd, wsem.at[6])
    for n, (src, dst) in enumerate(((x_hbm, x_ref), (ga_hbm, ga_ref), (gm_hbm, gm_ref), (turn_hbm, turn_ref))):
        loads["small", n] = pltpu.make_async_copy(src, dst, wsem.at[7 + n])
    last = []
    for n in range(U // ULAST):
        places = pl.ds(n * ULAST, ULAST)
        last.append(pltpu.make_async_copy(v_hbm.at[pl.ds(B - Q, Q), places], vbuf.at[(G - 1) % NS, :, places], lastsem.at[n]))

    def scatter(c, stage, rows, src, dst, s):
        return pltpu.make_async_remote_copy(src.at[at(s), rows], dst.at[s, rows], send_sem.at[stage], recv_sem.at[c, stage],
                                            device_id={"tp": at(s)}, device_id_type=MESH)

    def gather(c, stage, rows, buf, s):
        return pltpu.make_async_remote_copy(buf.at[me, rows], buf.at[me, rows], send_sem.at[stage], recv_sem.at[c, stage],
                                            device_id={"tp": at(s)}, device_id_type=MESH)

    def all_seven(c, stage, rows, buf):
        seven = buf.at[pl.ds(1, N - 1), rows]
        return pltpu.make_async_remote_copy(seven, seven, send_sem.at[stage], recv_sem.at[c, stage],
                                            device_id={"tp": at(1)}, device_id_type=MESH)

    others = (6, 7, 4, 5, 2, 3, 1)

    def part_rows(c):
        return pl.ds(PARTS[c][0] * Q, PARTS[c][1] * Q)

    def group_rows(c):
        return pl.ds(*GROUPS[c])

    with jax.named_scope("head"):
        for n in range(4):
            loads["small", n].start()
        loads["wq"].start()
        kcopy(0, 0).start()
        barrier = pltpu.get_barrier_semaphore()
        for s in range(1, N):
            pl.semaphore_signal(barrier, inc=1, device_id={"tp": at(s)}, device_id_type=MESH)
        for n in range(4):
            loads["small", n].wait()
        wide = x_ref[...].astype(F32)
        scale = lax.rsqrt(jnp.mean(wide * wide, -1, keepdims=True) + 1e-6)
        a = (wide * scale * row(ga_ref[...].astype(F32))).astype(BF16)
        loads["wq"].wait()
        kcopy(1, 1).start()
        kcopy(2, 2).start()
        vcopy(0, 0).start()
        vcopy(1, 1).start()
        loads["wo"].start()
        q = dot(a, wq[...]).astype(BF16).astype(F32)

    def picks(shape, row_axis, first):
        r = lax.broadcasted_iota(jnp.int32, shape, row_axis)
        s = lax.broadcasted_iota(jnp.int32, shape, 1 - row_axis) + first * Q
        rr = r % 16
        gg = r // 16 + first
        return [((s == gg * Q + rr - h * Q) & (rr >= h * Q) & (rr < (h + 1) * Q)).astype(BF16) for h in range(QUERIES)]

    with jax.named_scope("queries"):
        qa = jnp.zeros((16 * G, HEAD), F32)
        for h, pick in enumerate(picks((16 * G, B), 0, 0)):
            qh = q[:, h * HEAD : (h + 1) * HEAD]
            qa += dot(pick, (qh * turn_ref[0:1] + pltpu.roll(qh, HEAD // 2, 1) * turn_ref[1:2]).astype(BF16))
        block = lax.broadcasted_iota(jnp.int32, (16 * G, HEAD), 0) % Q
        for i in range(Q):
            qblk[:, i * HEAD : (i + 1) * HEAD] = jnp.where(block == i, qa, 0.0).astype(BF16)
    block = lax.broadcasted_iota(jnp.int32, (16, HEAD), 0) % Q

    def quad_rows(g):
        return pl.ds(pl.multiple_of(g * 16, 16), 16)

    def scores(g, slot, to):
        ql = qblk[quad_rows(g), :]
        for u in range(0, U, UC):
            kc = jnp.concatenate([kbuf[slot, i, u : u + UC, :] for i in range(Q)], axis=1)
            sbuf[to, :, u : u + UC] = lax.dot_general(ql, kc, (((1,), (1,)), ((), ())), preferred_element_type=F32)

    def softmax(of):
        s = sbuf[of]
        p = jnp.exp2((s - jnp.max(s, axis=1, keepdims=True)) * (HEAD**-0.5 * math.log2(math.e)))
        return (p * (1.0 / jnp.sum(p, axis=1, keepdims=True))).astype(BF16)

    def values(slot, w, first, places):
        o = jnp.zeros((16, Q * HEAD), F32)
        for u in range(first, first + places, UC):
            o += dot(w[:, u : u + UC], jnp.concatenate([vbuf[slot, i, u : u + UC, :] for i in range(Q)], axis=1))
        return o

    def keep(g, o):
        t = jnp.zeros((16, HEAD), F32)
        for i in range(Q):
            t = jnp.where(block == i, o[:, i * HEAD : (i + 1) * HEAD], t)
        oall[quad_rows(g), :] = t.astype(BF16)

    def terms(c, stage, rows, a, w_ref, part, recv):
        for n in range(4):
            t = dot(a, w_ref[:, n * 2 * W : (n + 1) * 2 * W])
            for j in range(2):
                own[2 * n + j, rows] = t[:, j * W : (j + 1) * W]
                part[2 * n + j, rows] = t[:, j * W : (j + 1) * W].astype(BF16)
        for s in others:
            scatter(c, stage, rows, part, recv, s).start()

    def finish(c):
        first, quads, _ = PARTS[c]
        o = oall[first * 16 : (first + quads) * 16, :]
        seen = [dot(pick, o).astype(BF16) for pick in picks((quads * Q, quads * 16), 1, first)]
        if c == 0:
            loads["wo"].wait()
            pl.semaphore_wait(barrier, N - 1)
        terms(c, 0, part_rows(c), jnp.concatenate(seen, axis=1), wo, part1, recv1)

    def summed(c, stage, rows, part, recv):
        all_seven(c, stage, rows, recv).wait_recv()
        t = own[me, rows]
        for s in range(1, N):
            t += recv[s, rows].astype(F32)
        return t

    def reduce1(c):
        rows = part_rows(c)
        mine = x_ref[rows, pl.ds(pl.multiple_of(me * W, 128), W)].astype(F32)
        hbuf[me, rows] = (mine + summed(c, 0, rows, part1, recv1)).astype(BF16)
        for s in others:
            gather(c, 1, rows, hbuf, s).start()

    def reduce2(c):
        rows = group_rows(c)
        ybuf[me, rows] = (hbuf[me, rows].astype(F32) + summed(c, 2, rows, part2, recv2)).astype(BF16)
        for s in others:
            gather(c, 3, rows, ybuf, s).start()

    def norm2(c, parts):
        for p in parts:
            all_seven(p, 1, part_rows(p), hbuf).wait_recv()
        rows = group_rows(c)
        squares = jnp.zeros((GROUPS[c][1], 1), F32)
        for j in range(N):
            t = hbuf[j, rows].astype(F32)
            squares += jnp.sum(t * t, -1, keepdims=True)
        scale = lax.rsqrt(squares * (1.0 / D) + 1e-6)
        gain = row(gm_ref[...].astype(F32))
        for j in range(N):
            bbuf[rows, j * W : (j + 1) * W] = (hbuf[j, rows].astype(F32) * scale * gain[:, j * W : (j + 1) * W]).astype(BF16)

    def hidden(c, n):
        rows = group_rows(c)
        if c == 0:
            loads["wg", n].wait()
            loads["wu", n].wait()
        b = bbuf[rows, :]
        gate = dot(b, wg[:, n * half : (n + 1) * half])
        up = dot(b, wu[:, n * half : (n + 1) * half])
        hid[rows, n * half : (n + 1) * half] = (jax.nn.silu(gate) * up).astype(BF16)

    def down(c):
        rows = group_rows(c)
        if c == 0:
            loads["wd"].wait()
        terms(c, 2, rows, hid[rows, :], wd, part2, recv2)

    with jax.named_scope("k0wait"):
        kcopy(0, 0).wait()
    scores(0, 0, 0)
    kcopy(3, 0).start()
    with jax.named_scope("k1wait"):
        kcopy(1, 1).wait()
    wbuf[0] = softmax(0)
    scores(1, 1, 1)

    def body(g, _):
        kslot, vslot = lax.rem(g + 2, NS), lax.rem(g, NS)
        with jax.named_scope("loopwait"):
            kcopy(g + 2, kslot).wait()
            vcopy(g, vslot).wait()

        @pl.when(g + 4 < G)
        def _():
            kcopy(g + 4, lax.rem(g + 4, NS)).start()

        @pl.when(g + 2 < G - 1)
        def _():
            vcopy(g + 2, lax.rem(g + 2, NS)).start()

        @pl.when(g + 2 == G - 1)
        def _():
            for copy in last:
                copy.start()
            for n in range(2):
                loads["wg", n].start(priority=1)
                loads["wu", n].start(priority=1)
            loads["wd"].start(priority=1)

        keep(g, values(vslot, wbuf.at[lax.rem(g, 2)], 0, U))
        wbuf[lax.rem(g + 1, 2)] = softmax(lax.rem(g + 1, NS))
        scores(g + 2, kslot, kslot)

        for c, (first, quads, reduced) in enumerate(PARTS[:-1]):
            @pl.when(g == first + quads - 1)
            def _(c=c):
                with jax.named_scope(f"finish{c}"):
                    finish(c)

            if reduced is not None:
                @pl.when(g == reduced)
                def _(c=c):
                    with jax.named_scope(f"reduce1_{c}"):
                        reduce1(c)

        return 0

    with jax.named_scope("loop"):
        lax.fori_loop(0, G - 2, body, 0)
    with jax.named_scope("v14"):
        vcopy(G - 2, (G - 2) % NS).wait()
    keep(G - 2, values((G - 2) % NS, wbuf.at[(G - 2) % 2], 0, U))
    wbuf[(G - 1) % 2] = softmax((G - 1) % NS)
    o = jnp.zeros((16, Q * HEAD), F32)
    for n, copy in enumerate(last):
        with jax.named_scope(f"last{n}"):
            copy.wait()
        o += values((G - 1) % NS, wbuf.at[(G - 1) % 2], n * ULAST, ULAST)
    keep(G - 1, o)
    with jax.named_scope("f2"):
        finish(2)
    with jax.named_scope("n0"):
        norm2(0, (0, 1))
    with jax.named_scope("h00"):
        hidden(0, 0)
    with jax.named_scope("r12"):
        reduce1(2)
    with jax.named_scope("h01"):
        hidden(0, 1)
    with jax.named_scope("d0"):
        down(0)
    with jax.named_scope("n1"):
        norm2(1, (2,))
    with jax.named_scope("h10"):
        hidden(1, 0)
    with jax.named_scope("h11"):
        hidden(1, 1)
    with jax.named_scope("d1"):
        down(1)
    with jax.named_scope("r20"):
        reduce2(0)
    with jax.named_scope("r21"):
        reduce2(1)
    for c in range(len(GROUPS)):
        rows = group_rows(c)
        with jax.named_scope(f"out{c}"):
            all_seven(c, 3, rows, ybuf).wait_recv()
        for j in range(N):
            out_ref[rows, j * W : (j + 1) * W] = ybuf[j, rows]
    with jax.named_scope("sent"):
        for stage, buf in enumerate((part1, hbuf, part2, ybuf)):
            all_seven(0, stage, pl.ds(0, B), buf).wait_send()


def solution(mesh):
    any_, vmem = pl.BlockSpec(memory_space=pl.ANY), pl.BlockSpec(memory_space=pltpu.VMEM)

    def step(x, k_cache, v_cache, gain_a, wq, wo, gain_m, w_gate, w_up, w_down):
        return pl.pallas_call(
            layer,
            out_shape=pltpu.VMEM((B, D), BF16),
            in_specs=[any_] * 11,
            out_specs=vmem,
            scratch_shapes=[
                pltpu.VMEM((B, D), BF16),
                pltpu.VMEM((D // 128, 128), BF16),
                pltpu.VMEM((D // 128, 128), BF16),
                pltpu.VMEM((2, HEAD), F32),
                pltpu.VMEM((NS, Q, U, HEAD), BF16),
                pltpu.VMEM((NS, Q, U, HEAD), BF16),
                pltpu.VMEM((D, QUERIES * HEAD), BF16),
                pltpu.VMEM((QUERIES * HEAD, D), BF16),
                pltpu.VMEM((D, HID), BF16),
                pltpu.VMEM((D, HID), BF16),
                pltpu.VMEM((HID, D), BF16),
                pltpu.VMEM((16 * G, Q * HEAD), BF16),
                pltpu.VMEM((NS, 16, U), F32),
                pltpu.VMEM((2, 16, U), BF16),
                pltpu.VMEM((16 * G, HEAD), BF16),
                pltpu.VMEM((B, D), BF16),
                pltpu.VMEM((B, HID), BF16),
                pltpu.VMEM((N, B, W), F32),
                *[pltpu.VMEM((N, B, W), BF16)] * 6,
                pltpu.SemaphoreType.DMA((NS,)),
                pltpu.SemaphoreType.DMA((NS,)),
                pltpu.SemaphoreType.DMA((U // ULAST,)),
                pltpu.SemaphoreType.DMA((11,)),
                pltpu.SemaphoreType.DMA((4,)),
                pltpu.SemaphoreType.DMA((len(PARTS), 4)),
            ],
            compiler_params=pltpu.CompilerParams(collective_id=0, has_side_effects=True, vmem_limit_bytes=56 * 2**20),
            name="layer",
        )(x, gain_a.reshape(-1, 128), gain_m.reshape(-1, 128), jnp.asarray(rotary_tables()), wq, wo, w_gate, w_up, w_down,
          k_cache.reshape(B, U, HEAD), v_cache.reshape(B, U, HEAD))

    states, cache, columns, rows_of = P("dp", None), P("dp", None, "tp", None), P(None, "tp"), P("tp", None)
    return jax.shard_map(
        step,
        mesh=mesh,
        in_specs=(states, cache, cache, P(None), columns, rows_of, P(None), columns, columns, rows_of),
        out_specs=states,
        check_vma=False,
    )
```

```python
import math

import jax
import jax.numpy as jnp
import numpy as np
from jax import lax
from jax.experimental import pallas as pl
from jax.experimental.pallas import tpu as pltpu
from jax.sharding import PartitionSpec as P

HEAD = 128
THETA = 10000
D = 3072
B = 64
U = 4096
Q = 4
G = B // Q
NS = 3
VS = 4
LEAD = 3
UC = 512
ULAST = 1024
N = 8
W = D // N
HID = 1024
PARTS = ((0, 8, 9), (8, 4, None), (12, 4, None))
GROUPS = ((0, 48), (48, 16))
QUERIES = 3
FAR_FIRST = ((3, 2), (1, 0))
F32, BF16 = jnp.float32, jnp.bfloat16
MESH = pl.DeviceIdType.MESH


def rotary_tables():
    half = HEAD // 2
    angle = (U - 1) * THETA ** (-np.arange(half, dtype=np.float64) / half)
    cos, sin = np.cos(angle), np.sin(angle)
    return np.stack([np.concatenate([cos, cos]), np.concatenate([-sin, sin])]).astype(np.float32)


def row(gain):
    return jnp.concatenate([gain[i : i + 1] for i in range(gain.shape[0])], axis=1)


def dot(a, b):
    return jnp.dot(a, b, preferred_element_type=F32)


def layer(x_hbm, ga_hbm, gm_hbm, turn_hbm, wq_hbm, wo_hbm, wg_hbm, wu_hbm, wd_hbm, k_hbm, v_hbm, out_ref,
          x_ref, ga_ref, gm_ref, turn_ref, kbuf, vbuf, wq, wo, wg, wu, wd, qblk, sbuf, wbuf, oall, bbuf, hid, own, part1, part2, recv1, recv2, hbuf, ybuf,
          ksem, vsem, lastsem, wsem, send_sem, recv_sem):
    me = lax.axis_index("tp")
    mx, my, mc = me // 4, lax.rem(me // 2, 2), lax.rem(me, 2)

    def chip(k):
        return 2 * lax.rem(mx + k // 2, 2) + lax.rem(my + k % 2, 2)

    def at(s):
        return 2 * chip(s // 2) + lax.rem(mc + s % 2, 2)

    def chip_columns(k):
        return pl.ds(pl.multiple_of(chip(k) * (2 * W), 128), 2 * W)

    def kcopy(g, slot):
        return pltpu.make_async_copy(k_hbm.at[pl.ds(g * Q, Q)], kbuf.at[slot], ksem.at[slot])

    def vcopy(g, slot):
        return pltpu.make_async_copy(v_hbm.at[pl.ds(g * Q, Q)], vbuf.at[slot], vsem.at[slot])

    half = HID // 2
    loads = {"wq": pltpu.make_async_copy(wq_hbm, wq, wsem.at[4]), "wo": pltpu.make_async_copy(wo_hbm, wo, wsem.at[3])}
    for n in range(2):
        cols = pl.ds(n * half, half)
        loads["wg", n] = pltpu.make_async_copy(wg_hbm.at[:, cols], wg.at[:, cols], wsem.at[n])
        loads["wu", n] = pltpu.make_async_copy(wu_hbm.at[:, cols], wu.at[:, cols], wsem.at[n])
    for h, ks in enumerate(FAR_FIRST):
        for k in ks:
            cols = chip_columns(k)
            loads["wd", k] = pltpu.make_async_copy(wd_hbm.at[:, cols], wd.at[:, cols], wsem.at[2 + h])
    down_halves = [pltpu.make_async_copy(wd_hbm.at[:, pl.ds(0, D // 2)], wd.at[:, pl.ds(0, D // 2)], wsem.at[2 + h]) for h in range(2)]
    for n, (src, dst) in enumerate(((x_hbm, x_ref), (ga_hbm, ga_ref), (gm_hbm, gm_ref), (turn_hbm, turn_ref))):
        loads["small", n] = pltpu.make_async_copy(src, dst, wsem.at[n])

    def both_halves(n):
        return pltpu.make_async_copy(wg_hbm, wg, wsem.at[n])

    last = []
    for n in range(U // ULAST):
        places = pl.ds(n * ULAST, ULAST)
        last.append(pltpu.make_async_copy(v_hbm.at[pl.ds(B - Q, Q), places], vbuf.at[(G - 1) % VS, :, places], lastsem.at[n]))

    def scatter(c, stage, rows, src, dst, s):
        return pltpu.make_async_remote_copy(src.at[at(s), rows], dst.at[s, rows], send_sem.at[stage], recv_sem.at[c, stage],
                                            device_id={"tp": at(s)}, device_id_type=MESH)

    def gather(c, stage, rows, buf, s):
        return pltpu.make_async_remote_copy(buf.at[me, rows], buf.at[me, rows], send_sem.at[stage], recv_sem.at[c, stage],
                                            device_id={"tp": at(s)}, device_id_type=MESH)

    def all_seven(c, stage, rows, buf):
        seven = buf.at[pl.ds(1, N - 1), rows]
        return pltpu.make_async_remote_copy(seven, seven, send_sem.at[stage], recv_sem.at[c, stage],
                                            device_id={"tp": at(1)}, device_id_type=MESH)

    others = (6, 7, 4, 5, 2, 3, 1)

    def part_rows(c):
        return pl.ds(PARTS[c][0] * Q, PARTS[c][1] * Q)

    def group_rows(c):
        return pl.ds(*GROUPS[c])

    with jax.named_scope("head"):
        for n in range(4):
            loads["small", n].start()
        loads["wq"].start()
        kcopy(0, 0).start()
        barrier = pltpu.get_barrier_semaphore()
        for s in range(1, N):
            pl.semaphore_signal(barrier, inc=1, device_id={"tp": at(s)}, device_id_type=MESH)
        for n in range(4):
            loads["small", n].wait()
        wide = x_ref[...].astype(F32)
        scale = lax.rsqrt(jnp.mean(wide * wide, -1, keepdims=True) + 1e-6)
        a = (wide * scale * row(ga_ref[...].astype(F32))).astype(BF16)
        loads["wq"].wait()
        kcopy(1, 1).start()
        kcopy(2, 2).start()
        vcopy(0, 0).start()
        vcopy(1, 1).start()
        loads["wo"].start()
        q = dot(a, wq[...]).astype(BF16).astype(F32)

    def picks(shape, row_axis, first):
        r = lax.broadcasted_iota(jnp.int32, shape, row_axis)
        s = lax.broadcasted_iota(jnp.int32, shape, 1 - row_axis) + first * Q
        rr = r % 16
        gg = r // 16 + first
        return [((s == gg * Q + rr - h * Q) & (rr >= h * Q) & (rr < (h + 1) * Q)).astype(BF16) for h in range(QUERIES)]

    with jax.named_scope("queries"):
        qa = jnp.zeros((16 * G, HEAD), F32)
        for h, pick in enumerate(picks((16 * G, B), 0, 0)):
            qh = q[:, h * HEAD : (h + 1) * HEAD]
            qa += dot(pick, (qh * turn_ref[0:1] + pltpu.roll(qh, HEAD // 2, 1) * turn_ref[1:2]).astype(BF16))
        block = lax.broadcasted_iota(jnp.int32, (16 * G, HEAD), 0) % Q
        for i in range(Q):
            qblk[:, i * HEAD : (i + 1) * HEAD] = jnp.where(block == i, qa, 0.0).astype(BF16)
    block = lax.broadcasted_iota(jnp.int32, (16, HEAD), 0) % Q

    def quad_rows(g):
        return pl.ds(pl.multiple_of(g * 16, 16), 16)

    def scores(g, slot, to):
        ql = qblk[quad_rows(g), :]
        for u in range(0, U, UC):
            kc = jnp.concatenate([kbuf[slot, i, u : u + UC, :] for i in range(Q)], axis=1)
            sbuf[to, :, u : u + UC] = lax.dot_general(ql, kc, (((1,), (1,)), ((), ())), preferred_element_type=F32)

    def softmax(of):
        s = sbuf[of]
        p = jnp.exp2((s - jnp.max(s, axis=1, keepdims=True)) * (HEAD**-0.5 * math.log2(math.e)))
        return (p * (1.0 / jnp.sum(p, axis=1, keepdims=True))).astype(BF16)

    def values(slot, w, first, places):
        o = jnp.zeros((16, Q * HEAD), F32)
        for u in range(first, first + places, UC):
            o += dot(w[:, u : u + UC], jnp.concatenate([vbuf[slot, i, u : u + UC, :] for i in range(Q)], axis=1))
        return o

    def keep(g, o):
        t = jnp.zeros((16, HEAD), F32)
        for i in range(Q):
            t = jnp.where(block == i, o[:, i * HEAD : (i + 1) * HEAD], t)
        oall[quad_rows(g), :] = t.astype(BF16)

    def terms(c, stage, rows, a, w_ref, part, recv, ready=None):
        for h, ks in enumerate(FAR_FIRST):
            if ready is not None:
                ready[h].wait()
            for k in ks:
                t = dot(a, w_ref[:, chip_columns(k)])
                for j in range(2):
                    own[2 * chip(k) + j, rows] = t[:, j * W : (j + 1) * W]
                    part[2 * chip(k) + j, rows] = t[:, j * W : (j + 1) * W].astype(BF16)
            for s in [2 * k + j for k in ks for j in range(2)]:
                if s:
                    scatter(c, stage, rows, part, recv, s).start()

    def finish(c):
        first, quads, _ = PARTS[c]
        o = oall[first * 16 : (first + quads) * 16, :]
        seen = [dot(pick, o).astype(BF16) for pick in picks((quads * Q, quads * 16), 1, first)]
        if c == 0:
            loads["wo"].wait()
            pl.semaphore_wait(barrier, N - 1)
        terms(c, 0, part_rows(c), jnp.concatenate(seen, axis=1), wo, part1, recv1)

    def summed(c, stage, rows, part, recv):
        all_seven(c, stage, rows, recv).wait_recv()
        t = own[me, rows]
        for s in range(1, N):
            t += recv[s, rows].astype(F32)
        return t

    def reduce1(c):
        rows = part_rows(c)
        mine = x_ref[rows, pl.ds(pl.multiple_of(me * W, 128), W)].astype(F32)
        hbuf[me, rows] = (mine + summed(c, 0, rows, part1, recv1)).astype(BF16)
        for s in others:
            gather(c, 1, rows, hbuf, s).start()

    def reduce2(c):
        rows = group_rows(c)
        ybuf[me, rows] = (hbuf[me, rows].astype(F32) + summed(c, 2, rows, part2, recv2)).astype(BF16)
        if c == 0:
            for k in (3, 2, 1):
                gather(0, 3, rows, ybuf, 2 * k).start()
            across(0).start()
        else:
            for s in others:
                gather(c, 3, rows, ybuf, s).start()

    def across(k):
        block = ybuf.at[2 * chip(k) + mc, group_rows(0)]
        return pltpu.make_async_remote_copy(block, block, send_sem.at[3], recv_sem.at[2, 3], device_id={"tp": at(1)}, device_id_type=MESH)

    def some(n, c, stage, rows, buf):
        blocks = buf.at[pl.ds(0, n), rows]
        return pltpu.make_async_remote_copy(blocks, blocks, send_sem.at[stage], recv_sem.at[c, stage],
                                            device_id={"tp": at(1)}, device_id_type=MESH)

    def norm2(c):
        rows = part_rows(c)
        all_seven(c, 1, rows, hbuf).wait_recv()
        squares = jnp.zeros((PARTS[c][1] * Q, 1), F32)
        for j in range(N):
            t = hbuf[j, rows].astype(F32)
            squares += jnp.sum(t * t, -1, keepdims=True)
        scale = lax.rsqrt(squares * (1.0 / D) + 1e-6)
        gain = row(gm_ref[...].astype(F32))
        for j in range(N):
            bbuf[rows, j * W : (j + 1) * W] = (hbuf[j, rows].astype(F32) * scale * gain[:, j * W : (j + 1) * W]).astype(BF16)

    def hidden(c, first, width):
        rows, cols = group_rows(c), pl.ds(first, width)
        b = bbuf[rows, :]
        hid[rows, cols] = (jax.nn.silu(dot(b, wg[:, cols])) * dot(b, wu[:, cols])).astype(BF16)

    def down(c):
        rows = group_rows(c)
        terms(c, 2, rows, hid[rows, :], wd, part2, recv2, down_halves if c == 0 else None)

    with jax.named_scope("k0wait"):
        kcopy(0, 0).wait()
    scores(0, 0, 0)
    kcopy(3, 0).start()
    wbuf[0] = softmax(0)
    with jax.named_scope("k1wait"):
        kcopy(1, 1).wait()
    scores(1, 1, 1)
    kcopy(4, 1).start()
    with jax.named_scope("k2wait"):
        kcopy(2, 2).wait()
    scores(2, 2, 2)

    def attended(g):
        keep(g, values(lax.rem(g, VS), wbuf.at[lax.rem(g, 2)], 0, U))
        wbuf[lax.rem(g + 1, 2)] = softmax(lax.rem(g + 1, LEAD + 1))

    def body(g, _):
        @pl.when(g + LEAD + 2 < G)
        def _():
            kcopy(g + LEAD + 2, lax.rem(g + LEAD + 2, NS)).start()

        vcopy(g + 2, lax.rem(g + 2, VS)).start()
        kslot = lax.rem(g + LEAD, NS)
        with jax.named_scope("loopwait"):
            kcopy(g + LEAD, kslot).wait()
            vcopy(g, lax.rem(g, VS)).wait()

        @pl.when(g == G - LEAD - 1)
        def _():
            for copy in last:
                copy.start()

        attended(g)
        scores(g + LEAD, kslot, lax.rem(g + LEAD, LEAD + 1))

        for c, (first, quads, reduced) in enumerate(PARTS[:-1]):
            @pl.when(g == first + quads - 1)
            def _(c=c):
                with jax.named_scope(f"finish{c}"):
                    finish(c)

            if reduced is not None:
                @pl.when(g == reduced)
                def _(c=c):
                    with jax.named_scope(f"reduce1_{c}"):
                        reduce1(c)

        return 0

    with jax.named_scope("loop"):
        lax.fori_loop(0, G - LEAD, body, 0)
    for g in range(G - LEAD, G - 1):
        with jax.named_scope(f"v{g}"):
            vcopy(g, g % VS).wait()
        attended(g)
    for n in range(2):
        loads["wg", n].start()
        loads["wu", n].start()
    for ks in FAR_FIRST:
        for k in ks:
            loads["wd", k].start()
    with jax.named_scope("r11"):
        reduce1(1)
    o = jnp.zeros((16, Q * HEAD), F32)
    for n, copy in enumerate(last):
        with jax.named_scope(f"last{n}"):
            copy.wait()
        o += values((G - 1) % VS, wbuf.at[(G - 1) % 2], n * ULAST, ULAST)
    keep(G - 1, o)
    with jax.named_scope("f2"):
        finish(2)
    with jax.named_scope("n0"):
        norm2(0)
    with jax.named_scope("n01"):
        norm2(1)
    with jax.named_scope("h00"):
        both_halves(0).wait()
        hidden(0, 0 * half, half)
    with jax.named_scope("r12"):
        reduce1(2)
    with jax.named_scope("h01"):
        both_halves(1).wait()
        hidden(0, 1 * half, half)
    with jax.named_scope("d0"):
        down(0)
    with jax.named_scope("n1"):
        norm2(2)
    with jax.named_scope("h1"):
        hidden(1, 0, HID)
    with jax.named_scope("d1"):
        down(1)
    with jax.named_scope("r20"):
        reduce2(0)
    with jax.named_scope("r21"):
        reduce2(1)
    with jax.named_scope("across"):
        some(N // 2 - 1, 0, 3, group_rows(0), ybuf).wait_recv()
        for k in (3, 2, 1):
            across(k).start()

    def put(c):
        rows = group_rows(c)
        for j in range(N):
            out_ref[rows, j * W : (j + 1) * W] = ybuf[j, rows]

    with jax.named_scope("out0"):
        some(N // 2, 2, 3, group_rows(0), ybuf).wait_recv()
    put(0)
    with jax.named_scope("out1"):
        all_seven(1, 3, group_rows(1), ybuf).wait_recv()
    put(1)
    with jax.named_scope("sent"):
        for stage, buf in enumerate((part1, hbuf, part2, ybuf)):
            all_seven(0, stage, pl.ds(0, B), buf).wait_send()


def solution(mesh):
    any_, vmem = pl.BlockSpec(memory_space=pl.ANY), pl.BlockSpec(memory_space=pltpu.VMEM)

    def step(x, k_cache, v_cache, gain_a, wq, wo, gain_m, w_gate, w_up, w_down):
        return pl.pallas_call(
            layer,
            out_shape=pltpu.VMEM((B, D), BF16),
            in_specs=[any_] * 11,
            out_specs=vmem,
            scratch_shapes=[
                pltpu.VMEM((B, D), BF16),
                pltpu.VMEM((D // 128, 128), BF16),
                pltpu.VMEM((D // 128, 128), BF16),
                pltpu.VMEM((2, HEAD), F32),
                pltpu.VMEM((NS, Q, U, HEAD), BF16),
                pltpu.VMEM((VS, Q, U, HEAD), BF16),
                pltpu.VMEM((D, QUERIES * HEAD), BF16),
                pltpu.VMEM((QUERIES * HEAD, D), BF16),
                pltpu.VMEM((D, HID), BF16),
                pltpu.VMEM((D, HID), BF16),
                pltpu.VMEM((HID, D), BF16),
                pltpu.VMEM((16 * G, Q * HEAD), BF16),
                pltpu.VMEM((LEAD + 1, 16, U), F32),
                pltpu.VMEM((2, 16, U), BF16),
                pltpu.VMEM((16 * G, HEAD), BF16),
                pltpu.VMEM((B, D), BF16),
                pltpu.VMEM((B, HID), BF16),
                pltpu.VMEM((N, B, W), F32),
                *[pltpu.VMEM((N, B, W), BF16)] * 6,
                pltpu.SemaphoreType.DMA((NS,)),
                pltpu.SemaphoreType.DMA((VS,)),
                pltpu.SemaphoreType.DMA((U // ULAST,)),
                pltpu.SemaphoreType.DMA((5,)),
                pltpu.SemaphoreType.DMA((4,)),
                pltpu.SemaphoreType.DMA((len(PARTS), 4)),
            ],
            compiler_params=pltpu.CompilerParams(collective_id=0, has_side_effects=True, vmem_limit_bytes=60 * 2**20),
            name="layer",
        )(x, gain_a.reshape(-1, 128), gain_m.reshape(-1, 128), jnp.asarray(rotary_tables()), wq, wo, w_gate, w_up, w_down,
          k_cache.reshape(B, U, HEAD), v_cache.reshape(B, U, HEAD))

    states, cache, columns, rows_of = P("dp", None), P("dp", None, "tp", None), P(None, "tp"), P("tp", None)
    return jax.shard_map(
        step,
        mesh=mesh,
        in_specs=(states, cache, cache, P(None), columns, rows_of, P(None), columns, columns, rows_of),
        out_specs=states,
        check_vma=False,
    )
```

```python
import math

import jax
import jax.numpy as jnp
import numpy as np
from jax import lax
from jax.experimental import pallas as pl
from jax.experimental.pallas import tpu as pltpu
from jax.sharding import PartitionSpec as P

HEAD = 128
THETA = 10000
D = 3072
B = 64
U = 4096
Q = 4
G = B // Q
NS = 3
VS = 4
LEAD = 3
UC = 512
ULAST = 1024
N = 8
W = D // N
HID = 1024
PARTS = ((0, 8), (8, 4), (12, 4))
REDUCE_AT = 9
GROUPS = ((0, 48), (48, 16))
QUERIES = 3
FAR_FIRST = ((3, 2), (1, 0))
F32, BF16 = jnp.float32, jnp.bfloat16
MESH = pl.DeviceIdType.MESH


def rotary_tables():
    half = HEAD // 2
    angle = (U - 1) * THETA ** (-np.arange(half, dtype=np.float64) / half)
    cos, sin = np.cos(angle), np.sin(angle)
    return np.stack([np.concatenate([cos, cos]), np.concatenate([-sin, sin])]).astype(np.float32)


def row(gain):
    return jnp.concatenate([gain[i : i + 1] for i in range(gain.shape[0])], axis=1)


def dot(a, b):
    return jnp.dot(a, b, preferred_element_type=F32)


def layer(x_hbm, ga_hbm, gm_hbm, turn_hbm, wq_hbm, wo_hbm, wg_hbm, wu_hbm, wd_hbm, k_hbm, v_hbm, out_ref,
          x_ref, ga_ref, gm_ref, turn_ref, kbuf, vbuf, wq, wo, wg, wu, wd, qblk, sbuf, wbuf, seen, bbuf, hid, own, part1, part2, recv1, recv2, hbuf, ybuf,
          ksem, vsem, lastsem, wsem, send_sem, recv_sem):
    me = lax.axis_index("tp")
    mx, my, mc = me // 4, lax.rem(me // 2, 2), lax.rem(me, 2)

    def chip(k):
        return 2 * lax.rem(mx + k // 2, 2) + lax.rem(my + k % 2, 2)

    def at(s):
        return 2 * chip(s // 2) + lax.rem(mc + s % 2, 2)

    def chip_columns(k):
        return pl.ds(pl.multiple_of(chip(k) * (2 * W), 128), 2 * W)

    def kcopy(g, slot):
        return pltpu.make_async_copy(k_hbm.at[pl.ds(g * Q, Q)], kbuf.at[slot], ksem.at[slot])

    def vcopy(g, slot):
        return pltpu.make_async_copy(v_hbm.at[pl.ds(g * Q, Q)], vbuf.at[slot], vsem.at[slot])

    half = HID // 2
    loads = {"wq": pltpu.make_async_copy(wq_hbm, wq, wsem.at[4]), "wo": pltpu.make_async_copy(wo_hbm, wo, wsem.at[3])}
    for n in range(2):
        cols = pl.ds(n * half, half)
        loads["wg", n] = pltpu.make_async_copy(wg_hbm.at[:, cols], wg.at[:, cols], wsem.at[n])
        loads["wu", n] = pltpu.make_async_copy(wu_hbm.at[:, cols], wu.at[:, cols], wsem.at[n])
    for h, ks in enumerate(FAR_FIRST):
        for k in ks:
            cols = chip_columns(k)
            loads["wd", k] = pltpu.make_async_copy(wd_hbm.at[:, cols], wd.at[:, cols], wsem.at[2 + h])
    down_halves = [pltpu.make_async_copy(wd_hbm.at[:, pl.ds(0, D // 2)], wd.at[:, pl.ds(0, D // 2)], wsem.at[2 + h]) for h in range(2)]
    for n, (src, dst) in enumerate(((x_hbm, x_ref), (ga_hbm, ga_ref), (gm_hbm, gm_ref), (turn_hbm, turn_ref))):
        loads["small", n] = pltpu.make_async_copy(src, dst, wsem.at[n])

    def both_halves(n):
        return pltpu.make_async_copy(wg_hbm, wg, wsem.at[n])

    last = []
    for n in range(U // ULAST):
        places = pl.ds(n * ULAST, ULAST)
        last.append(pltpu.make_async_copy(v_hbm.at[pl.ds(B - Q, Q), places], vbuf.at[(G - 1) % VS, :, places], lastsem.at[n]))

    def scatter(c, stage, rows, src, dst, s):
        return pltpu.make_async_remote_copy(src.at[at(s), rows], dst.at[s, rows], send_sem.at[stage], recv_sem.at[c, stage],
                                            device_id={"tp": at(s)}, device_id_type=MESH)

    def gather(c, stage, rows, buf, s):
        return pltpu.make_async_remote_copy(buf.at[me, rows], buf.at[me, rows], send_sem.at[stage], recv_sem.at[c, stage],
                                            device_id={"tp": at(s)}, device_id_type=MESH)

    def all_seven(c, stage, rows, buf):
        seven = buf.at[pl.ds(1, N - 1), rows]
        return pltpu.make_async_remote_copy(seven, seven, send_sem.at[stage], recv_sem.at[c, stage],
                                            device_id={"tp": at(1)}, device_id_type=MESH)

    others = (6, 7, 4, 5, 2, 3, 1)

    def part_rows(c):
        return pl.ds(PARTS[c][0] * Q, PARTS[c][1] * Q)

    def group_rows(c):
        return pl.ds(*GROUPS[c])

    with jax.named_scope("head"):
        for n in range(4):
            loads["small", n].start()
        loads["wq"].start()
        kcopy(0, 0).start()
        barrier = pltpu.get_barrier_semaphore()
        for s in range(1, N):
            pl.semaphore_signal(barrier, inc=1, device_id={"tp": at(s)}, device_id_type=MESH)
        for n in range(4):
            loads["small", n].wait()
        wide = x_ref[...].astype(F32)
        scale = lax.rsqrt(jnp.mean(wide * wide, -1, keepdims=True) + 1e-6)
        a = (wide * scale * row(ga_ref[...].astype(F32))).astype(BF16)
        loads["wq"].wait()
        kcopy(1, 1).start()
        kcopy(2, 2).start()
        vcopy(0, 0).start()
        vcopy(1, 1).start()
        loads["wo"].start()
        q = dot(a, wq[...]).astype(BF16).astype(F32)

    def picks(shape, row_axis, first):
        r = lax.broadcasted_iota(jnp.int32, shape, row_axis)
        s = lax.broadcasted_iota(jnp.int32, shape, 1 - row_axis) + first * Q
        rr = r % 16
        gg = r // 16 + first
        return [((s == gg * Q + rr - h * Q) & (rr >= h * Q) & (rr < (h + 1) * Q)).astype(BF16) for h in range(QUERIES)]

    with jax.named_scope("queries"):
        qa = jnp.zeros((16 * G, HEAD), F32)
        for h, pick in enumerate(picks((16 * G, B), 0, 0)):
            qh = q[:, h * HEAD : (h + 1) * HEAD]
            qa += dot(pick, (qh * turn_ref[0:1] + pltpu.roll(qh, HEAD // 2, 1) * turn_ref[1:2]).astype(BF16))
        block = lax.broadcasted_iota(jnp.int32, (16 * G, HEAD), 0) % Q
        for i in range(Q):
            qblk[:, i * HEAD : (i + 1) * HEAD] = jnp.where(block == i, qa, 0.0).astype(BF16)
    block = lax.broadcasted_iota(jnp.int32, (16, HEAD), 0) % Q

    def quad_rows(g):
        return pl.ds(pl.multiple_of(g * 16, 16), 16)

    def scores(g, slot, to):
        ql = qblk[quad_rows(g), :]
        for u in range(0, U, UC):
            kc = jnp.concatenate([kbuf[slot, i, u : u + UC, :] for i in range(Q)], axis=1)
            sbuf[to, :, u : u + UC] = lax.dot_general(ql, kc, (((1,), (1,)), ((), ())), preferred_element_type=F32)

    def softmax(of):
        s = sbuf[of]
        p = jnp.exp2((s - jnp.max(s, axis=1, keepdims=True)) * (HEAD**-0.5 * math.log2(math.e)))
        return (p * (1.0 / jnp.sum(p, axis=1, keepdims=True))).astype(BF16)

    def values(slot, w, first, places):
        o = jnp.zeros((16, Q * HEAD), F32)
        for u in range(first, first + places, UC):
            o += dot(w[:, u : u + UC], jnp.concatenate([vbuf[slot, i, u : u + UC, :] for i in range(Q)], axis=1))
        return o

    def keep(g, o):
        t = jnp.zeros((16, HEAD), F32)
        for i in range(Q):
            t = jnp.where(block == i, o[:, i * HEAD : (i + 1) * HEAD], t)
        for h in range(QUERIES):
            seen[g, :, h * HEAD : (h + 1) * HEAD] = t[h * Q : (h + 1) * Q]

    def terms(c, stage, rows, a, w_ref, part, recv, ready=None):
        for h, ks in enumerate(FAR_FIRST):
            if ready is not None:
                ready[h].wait()
            for k in ks:
                t = dot(a, w_ref[:, chip_columns(k)])
                for j in range(2):
                    own[2 * chip(k) + j, rows] = t[:, j * W : (j + 1) * W]
                    part[2 * chip(k) + j, rows] = t[:, j * W : (j + 1) * W].astype(BF16)
            for s in [2 * k + j for k in ks for j in range(2)]:
                if s:
                    scatter(c, stage, rows, part, recv, s).start()

    def finish(c):
        if c == 0:
            loads["wo"].wait()
            pl.semaphore_wait(barrier, N - 1)
        first, quads = PARTS[c]
        rows = jnp.concatenate([seen[g] for g in range(first, first + quads)], axis=0).astype(BF16)
        terms(c, 0, part_rows(c), rows, wo, part1, recv1)

    def summed(c, stage, rows, part, recv):
        all_seven(c, stage, rows, recv).wait_recv()
        t = own[me, rows]
        for s in range(1, N):
            t += recv[s, rows].astype(F32)
        return t

    def reduce1(c):
        rows = part_rows(c)
        mine = x_ref[rows, pl.ds(pl.multiple_of(me * W, 128), W)].astype(F32)
        hbuf[me, rows] = (mine + summed(c, 0, rows, part1, recv1)).astype(BF16)
        for s in others:
            gather(c, 1, rows, hbuf, s).start()

    def reduce2(c):
        rows = group_rows(c)
        ybuf[me, rows] = (hbuf[me, rows].astype(F32) + summed(c, 2, rows, part2, recv2)).astype(BF16)
        if c == 0:
            for k in (3, 2, 1):
                gather(0, 3, rows, ybuf, 2 * k).start()
            across(0).start()
        else:
            for s in others:
                gather(c, 3, rows, ybuf, s).start()

    def across(k):
        block = ybuf.at[2 * chip(k) + mc, group_rows(0)]
        return pltpu.make_async_remote_copy(block, block, send_sem.at[3], recv_sem.at[2, 3], device_id={"tp": at(1)}, device_id_type=MESH)

    def some(n, c, stage, rows, buf):
        blocks = buf.at[pl.ds(0, n), rows]
        return pltpu.make_async_remote_copy(blocks, blocks, send_sem.at[stage], recv_sem.at[c, stage],
                                            device_id={"tp": at(1)}, device_id_type=MESH)

    def norm2(c):
        rows = part_rows(c)
        all_seven(c, 1, rows, hbuf).wait_recv()
        squares = jnp.zeros((PARTS[c][1] * Q, 1), F32)
        for j in range(N):
            t = hbuf[j, rows].astype(F32)
            squares += jnp.sum(t * t, -1, keepdims=True)
        scale = lax.rsqrt(squares * (1.0 / D) + 1e-6)
        gain = row(gm_ref[...].astype(F32))
        for j in range(N):
            bbuf[rows, j * W : (j + 1) * W] = (hbuf[j, rows].astype(F32) * scale * gain[:, j * W : (j + 1) * W]).astype(BF16)

    def hidden(c, first, width):
        rows, cols = group_rows(c), pl.ds(first, width)
        b = bbuf[rows, :]
        hid[rows, cols] = (jax.nn.silu(dot(b, wg[:, cols])) * dot(b, wu[:, cols])).astype(BF16)

    def down(c):
        rows = group_rows(c)
        terms(c, 2, rows, hid[rows, :], wd, part2, recv2, down_halves if c == 0 else None)

    with jax.named_scope("k0wait"):
        kcopy(0, 0).wait()
    scores(0, 0, 0)
    kcopy(3, 0).start()
    wbuf[0] = softmax(0)
    with jax.named_scope("k1wait"):
        kcopy(1, 1).wait()
    scores(1, 1, 1)
    kcopy(4, 1).start()
    with jax.named_scope("k2wait"):
        kcopy(2, 2).wait()
    scores(2, 2, 2)

    def mod(g, n):
        return g % n if isinstance(g, int) else lax.rem(g, n)

    def attended(g):
        keep(g, values(mod(g, VS), wbuf.at[mod(g, 2)], 0, U))
        wbuf[mod(g + 1, 2)] = softmax(mod(g + 1, LEAD + 1))

    def arrive(g):
        kcopy(g + LEAD, mod(g + LEAD, NS)).wait()
        vcopy(g, mod(g, VS)).wait()

    def ahead(g):
        scores(g + LEAD, mod(g + LEAD, NS), mod(g + LEAD, LEAD + 1))

    def body(g, _):
        @pl.when(g + LEAD + 2 < G)
        def _():
            kcopy(g + LEAD + 2, mod(g + LEAD + 2, NS)).start()

        vcopy(g + 2, mod(g + 2, VS)).start()
        with jax.named_scope("loopwait"):
            arrive(g)
        attended(g)
        ahead(g)

        @pl.when(g == PARTS[0][1] - 1)
        def _():
            with jax.named_scope("finish0"):
                finish(0)

        @pl.when(g == REDUCE_AT)
        def _():
            with jax.named_scope("reduce1_0"):
                reduce1(0)

        return 0

    with jax.named_scope("loop"):
        lax.fori_loop(0, G - LEAD - 2, body, 0)
    vcopy(G - LEAD, (G - LEAD) % VS).start()
    arrive(G - LEAD - 2)
    attended(G - LEAD - 2)
    with jax.named_scope("finish1"):
        finish(1)
    ahead(G - LEAD - 2)
    vcopy(G - LEAD + 1, (G - LEAD + 1) % VS).start()
    with jax.named_scope("arrive12"):
        arrive(G - LEAD - 1)
    for copy in last:
        copy.start()
    attended(G - LEAD - 1)
    ahead(G - LEAD - 1)
    with jax.named_scope("v13"):
        vcopy(G - LEAD, (G - LEAD) % VS).wait()
    attended(G - LEAD)
    with jax.named_scope("r11"):
        reduce1(1)
    with jax.named_scope("v14"):
        vcopy(G - LEAD + 1, (G - LEAD + 1) % VS).wait()
    attended(G - LEAD + 1)
    for n in range(2):
        loads["wg", n].start()
        loads["wu", n].start()
    for ks in FAR_FIRST:
        for k in ks:
            loads["wd", k].start()
    o = jnp.zeros((16, Q * HEAD), F32)
    for n, copy in enumerate(last):
        with jax.named_scope(f"last{n}"):
            copy.wait()
        o += values((G - 1) % VS, wbuf.at[(G - 1) % 2], n * ULAST, ULAST)
    keep(G - 1, o)
    with jax.named_scope("f2"):
        finish(2)
    with jax.named_scope("n0"):
        norm2(0)
    with jax.named_scope("n01"):
        norm2(1)
    with jax.named_scope("h00"):
        both_halves(0).wait()
        hidden(0, 0 * half, half)
    with jax.named_scope("r12"):
        reduce1(2)
    with jax.named_scope("h01"):
        both_halves(1).wait()
        hidden(0, 1 * half, half)
    with jax.named_scope("d0"):
        down(0)
    with jax.named_scope("n1"):
        norm2(2)
    with jax.named_scope("h1"):
        hidden(1, 0, HID)
    with jax.named_scope("d1"):
        down(1)
    with jax.named_scope("r20"):
        reduce2(0)
    with jax.named_scope("r21"):
        reduce2(1)
    with jax.named_scope("across"):
        some(N // 2 - 1, 0, 3, group_rows(0), ybuf).wait_recv()
        for k in (3, 2, 1):
            across(k).start()

    def put(c):
        rows = group_rows(c)
        for j in range(N):
            out_ref[rows, j * W : (j + 1) * W] = ybuf[j, rows]

    with jax.named_scope("out0"):
        some(N // 2, 2, 3, group_rows(0), ybuf).wait_recv()
    put(0)
    with jax.named_scope("out1"):
        all_seven(1, 3, group_rows(1), ybuf).wait_recv()
    put(1)
    with jax.named_scope("sent"):
        for stage, buf in enumerate((part1, hbuf, part2, ybuf)):
            all_seven(0, stage, pl.ds(0, B), buf).wait_send()


def solution(mesh):
    any_, vmem = pl.BlockSpec(memory_space=pl.ANY), pl.BlockSpec(memory_space=pltpu.VMEM)

    def step(x, k_cache, v_cache, gain_a, wq, wo, gain_m, w_gate, w_up, w_down):
        return pl.pallas_call(
            layer,
            out_shape=pltpu.VMEM((B, D), BF16),
            in_specs=[any_] * 11,
            out_specs=vmem,
            scratch_shapes=[
                pltpu.VMEM((B, D), BF16),
                pltpu.VMEM((D // 128, 128), BF16),
                pltpu.VMEM((D // 128, 128), BF16),
                pltpu.VMEM((2, HEAD), F32),
                pltpu.VMEM((NS, Q, U, HEAD), BF16),
                pltpu.VMEM((VS, Q, U, HEAD), BF16),
                pltpu.VMEM((D, QUERIES * HEAD), BF16),
                pltpu.VMEM((QUERIES * HEAD, D), BF16),
                pltpu.VMEM((D, HID), BF16),
                pltpu.VMEM((D, HID), BF16),
                pltpu.VMEM((HID, D), BF16),
                pltpu.VMEM((16 * G, Q * HEAD), BF16),
                pltpu.VMEM((LEAD + 1, 16, U), F32),
                pltpu.VMEM((2, 16, U), BF16),
                pltpu.VMEM((G, Q, QUERIES * HEAD), F32),
                pltpu.VMEM((B, D), BF16),
                pltpu.VMEM((B, HID), BF16),
                pltpu.VMEM((N, B, W), F32),
                *[pltpu.VMEM((N, B, W), BF16)] * 6,
                pltpu.SemaphoreType.DMA((NS,)),
                pltpu.SemaphoreType.DMA((VS,)),
                pltpu.SemaphoreType.DMA((U // ULAST,)),
                pltpu.SemaphoreType.DMA((5,)),
                pltpu.SemaphoreType.DMA((4,)),
                pltpu.SemaphoreType.DMA((len(PARTS), 4)),
            ],
            compiler_params=pltpu.CompilerParams(collective_id=0, has_side_effects=True, vmem_limit_bytes=60 * 2**20),
            name="layer",
        )(x, gain_a.reshape(-1, 128), gain_m.reshape(-1, 128), jnp.asarray(rotary_tables()), wq, wo, w_gate, w_up, w_down,
          k_cache.reshape(B, U, HEAD), v_cache.reshape(B, U, HEAD))

    states, cache, columns, rows_of = P("dp", None), P("dp", None, "tp", None), P(None, "tp"), P("tp", None)
    return jax.shard_map(
        step,
        mesh=mesh,
        in_specs=(states, cache, cache, P(None), columns, rows_of, P(None), columns, columns, rows_of),
        out_specs=states,
        check_vma=False,
    )
```

```python
import math

import jax
import jax.numpy as jnp
import numpy as np
from jax import lax
from jax.experimental import pallas as pl
from jax.experimental.pallas import tpu as pltpu
from jax.sharding import PartitionSpec as P

HEAD = 128
THETA = 10000
D = 3072
B = 64
U = 4096
Q = 4
G = B // Q
NS = 3
VS = 4
LEAD = 3
UC = 512
ULAST = 1024
N = 8
W = D // N
HID = 1024
PARTS = ((0, 8), (8, 4), (12, 4))
REDUCE_AT = 9
GROUPS = ((0, 48), (48, 16))
QUERIES = 3
FAR_FIRST = ((3, 2), (1, 0))
F32, BF16 = jnp.float32, jnp.bfloat16
MESH = pl.DeviceIdType.MESH


def rotary_tables():
    half = HEAD // 2
    angle = (U - 1) * THETA ** (-np.arange(half, dtype=np.float64) / half)
    cos, sin = np.cos(angle), np.sin(angle)
    return np.stack([np.concatenate([cos, cos]), np.concatenate([-sin, sin])]).astype(np.float32)


def row(gain):
    return jnp.concatenate([gain[i : i + 1] for i in range(gain.shape[0])], axis=1)


def dot(a, b):
    return jnp.dot(a, b, preferred_element_type=F32)


def layer(x_hbm, ga_hbm, gm_hbm, turn_hbm, wq_hbm, wo_hbm, wg_hbm, wu_hbm, wd_hbm, k_hbm, v_hbm, out_ref,
          x_ref, ga_ref, gm_ref, gain_m, turn_ref, kbuf, vbuf, wq, wo, wg, wu, wd, qblk, sbuf, wbuf, seen, bbuf, hid, own, part1, part2, recv1, recv2, hbuf, ybuf,
          ksem, vsem, wsem, send_sem, recv_sem):
    me = lax.axis_index("tp")
    mx, my, mc = me // 4, lax.rem(me // 2, 2), lax.rem(me, 2)

    here = me >= 0

    def chip(k):
        return 2 * lax.rem(mx + k // 2, 2) + lax.rem(my + k % 2, 2)

    def at(s):
        return 2 * chip(s // 2) + lax.rem(mc + s % 2, 2)

    def chip_columns(k):
        return pl.ds(pl.multiple_of(chip(k) * (2 * W), 128), 2 * W)

    def kcopy(g, slot):
        return pltpu.make_async_copy(k_hbm.at[pl.ds(g * Q, Q)], kbuf.at[slot], ksem.at[slot])

    def vcopy(g, slot):
        return pltpu.make_async_copy(v_hbm.at[pl.ds(g * Q, Q)], vbuf.at[slot], vsem.at[slot])

    half = HID // 2
    loads = {"wq": pltpu.make_async_copy(wq_hbm, wq, wsem.at[4]), "wo": pltpu.make_async_copy(wo_hbm, wo, wsem.at[3])}
    for n in range(2):
        cols = pl.ds(n * half, half)
        loads["wg", n] = pltpu.make_async_copy(wg_hbm.at[:, cols], wg.at[:, cols], wsem.at[n])
        loads["wu", n] = pltpu.make_async_copy(wu_hbm.at[:, cols], wu.at[:, cols], wsem.at[n])
    for h, ks in enumerate(FAR_FIRST):
        for k in ks:
            cols = chip_columns(k)
            loads["wd", k] = pltpu.make_async_copy(wd_hbm.at[:, cols], wd.at[:, cols], wsem.at[2 + h])
    down_halves = [pltpu.make_async_copy(wd_hbm.at[:, pl.ds(0, D // 2)], wd.at[:, pl.ds(0, D // 2)], wsem.at[2 + h]) for h in range(2)]
    for n, (src, dst) in enumerate(((x_hbm, x_ref), (ga_hbm, ga_ref), (gm_hbm, gm_ref), (turn_hbm, turn_ref))):
        loads["small", n] = pltpu.make_async_copy(src, dst, wsem.at[n])

    def both_halves(n):
        return pltpu.make_async_copy(wg_hbm, wg, wsem.at[n])

    last = []
    for n in range(U // ULAST):
        places = pl.ds(n * ULAST, ULAST)
        last.append(pltpu.make_async_copy(v_hbm.at[pl.ds(B - Q, Q), places], vbuf.at[(G - 1) % VS, :, places], ksem.at[n] if n < NS else wsem.at[4]))

    def arrivals(c, stage):
        return len(PARTS) * (stage % 2) + c

    def scatter(c, stage, rows, src, dst, s):
        return pltpu.make_async_remote_copy(src.at[at(s), rows], dst.at[s, rows], send_sem, recv_sem.at[arrivals(c, stage)],
                                            device_id={"tp": at(s)}, device_id_type=MESH)

    def gather(c, stage, rows, buf, s):
        return pltpu.make_async_remote_copy(buf.at[me, rows], buf.at[me, rows], send_sem, recv_sem.at[arrivals(c, stage)],
                                            device_id={"tp": at(s)}, device_id_type=MESH)

    def all_seven(c, stage, rows, buf):
        seven = buf.at[pl.ds(1, N - 1), rows]
        return pltpu.make_async_remote_copy(seven, seven, send_sem, recv_sem.at[arrivals(c, stage)],
                                            device_id={"tp": at(1)}, device_id_type=MESH)

    others = (6, 7, 4, 5, 2, 3, 1)

    def part_rows(c):
        return pl.ds(PARTS[c][0] * Q, PARTS[c][1] * Q)

    def group_rows(c):
        return pl.ds(*GROUPS[c])

    with jax.named_scope("head"):
        for n in range(4):
            loads["small", n].start()
        loads["wq"].start()
        kcopy(0, 0).start()
        barrier = pltpu.get_barrier_semaphore()
        for s in range(1, N):
            pl.semaphore_signal(barrier, inc=1, device_id={"tp": at(s)}, device_id_type=MESH)
        for n in range(4):
            loads["small", n].wait()
        wide = x_ref[...].astype(F32)
        scale = lax.rsqrt(jnp.mean(wide * wide, -1, keepdims=True) + 1e-6)
        a = (wide * scale * row(ga_ref[...].astype(F32))).astype(BF16)
        gain_m[...] = row(gm_ref[...].astype(F32))
        loads["wq"].wait()
        kcopy(1, 1).start()
        kcopy(2, 2).start()
        vcopy(0, 0).start()
        vcopy(1, 1).start()
        loads["wo"].start()
        q = dot(a, wq[...]).astype(BF16).astype(F32)

    def picks(shape, row_axis, first):
        r = lax.broadcasted_iota(jnp.int32, shape, row_axis)
        s = lax.broadcasted_iota(jnp.int32, shape, 1 - row_axis) + first * Q
        rr = r % 16
        gg = r // 16 + first
        return [((s == gg * Q + rr - h * Q) & (rr >= h * Q) & (rr < (h + 1) * Q)).astype(BF16) for h in range(QUERIES)]

    with jax.named_scope("queries"):
        qa = jnp.zeros((16 * G, HEAD), F32)
        for h, pick in enumerate(picks((16 * G, B), 0, 0)):
            qh = q[:, h * HEAD : (h + 1) * HEAD]
            qa += dot(pick, (qh * turn_ref[0:1] + pltpu.roll(qh, HEAD // 2, 1) * turn_ref[1:2]).astype(BF16))
        block = lax.broadcasted_iota(jnp.int32, (16 * G, HEAD), 0) % Q
        for i in range(Q):
            qblk[:, i * HEAD : (i + 1) * HEAD] = jnp.where(block == i, qa, 0.0).astype(BF16)
    block = lax.broadcasted_iota(jnp.int32, (16, HEAD), 0) % Q

    def quad_rows(g):
        return pl.ds(pl.multiple_of(g * 16, 16), 16)

    def scores(g, slot, to):
        ql = qblk[quad_rows(g), :]
        for u in range(0, U, UC):
            kc = jnp.concatenate([kbuf[slot, i, u : u + UC, :] for i in range(Q)], axis=1)
            sbuf[to, :, u : u + UC] = lax.dot_general(ql, kc, (((1,), (1,)), ((), ())), preferred_element_type=F32)

    def softmax(of):
        s = sbuf[of]
        p = jnp.exp2((s - jnp.max(s, axis=1, keepdims=True)) * (HEAD**-0.5 * math.log2(math.e)))
        return (p * (1.0 / jnp.sum(p, axis=1, keepdims=True))).astype(BF16)

    def values(slot, w, first, places):
        o = jnp.zeros((16, Q * HEAD), F32)
        for u in range(first, first + places, UC):
            o += dot(w[:, u : u + UC], jnp.concatenate([vbuf[slot, i, u : u + UC, :] for i in range(Q)], axis=1))
        return o

    def keep(g, o):
        t = jnp.zeros((16, HEAD), F32)
        for i in range(Q):
            t = jnp.where(block == i, o[:, i * HEAD : (i + 1) * HEAD], t)
        for h in range(QUERIES):
            seen[g, :, h * HEAD : (h + 1) * HEAD] = t[h * Q : (h + 1) * Q]

    def terms(c, stage, rows, a, w_ref, part, recv, ready=None):
        for h, ks in enumerate(FAR_FIRST):
            if ready is not None:
                ready[h].wait()
            for k in ks:
                t = dot(a, w_ref[:, chip_columns(k)])
                for j in range(2):
                    own[2 * chip(k) + j, rows] = t[:, j * W : (j + 1) * W]
                    part[2 * chip(k) + j, rows] = t[:, j * W : (j + 1) * W].astype(BF16)
            for s in [2 * k + j for k in ks for j in range(2)]:
                if s:
                    scatter(c, stage, rows, part, recv, s).start()

    def finish(c):
        if c == 0:
            loads["wo"].wait()
            pl.semaphore_wait(barrier, N - 1)
        first, quads = PARTS[c]
        rows = jnp.concatenate([seen[g] for g in range(first, first + quads)], axis=0).astype(BF16)
        terms(c, 0, part_rows(c), rows, wo, part1, recv1)

    def summed(c, stage, rows, part, recv):
        all_seven(c, stage, rows, recv).wait_recv()
        t = own[me, rows]
        for s in range(1, N):
            t += recv[s, rows].astype(F32)
        return t

    def reduce1(c):
        rows = part_rows(c)
        mine = x_ref[rows, pl.ds(pl.multiple_of(me * W, 128), W)].astype(F32)
        hbuf[me, rows] = (mine + summed(c, 0, rows, part1, recv1)).astype(BF16)
        for s in others:
            gather(c, 1, rows, hbuf, s).start()

    def reduce2(c):
        rows = group_rows(c)
        ybuf[me, rows] = (hbuf[me, rows].astype(F32) + summed(c, 2, rows, part2, recv2)).astype(BF16)
        if c == 0:
            for k in (3, 2, 1):
                gather(0, 3, rows, ybuf, 2 * k).start()
            across(0).start()
        else:
            for s in others:
                gather(c, 3, rows, ybuf, s).start()

    def across(k):
        block = ybuf.at[2 * chip(k) + mc, group_rows(0)]
        return pltpu.make_async_remote_copy(block, block, send_sem, recv_sem.at[2], device_id={"tp": at(1)}, device_id_type=MESH)

    def some(n, c, stage, rows, buf):
        blocks = buf.at[pl.ds(0, n), rows]
        return pltpu.make_async_remote_copy(blocks, blocks, send_sem, recv_sem.at[arrivals(c, stage)],
                                            device_id={"tp": at(1)}, device_id_type=MESH)

    def norm2(c):
        rows = part_rows(c)
        all_seven(c, 1, rows, hbuf).wait_recv()
        squares = jnp.zeros((PARTS[c][1] * Q, 1), F32)
        for j in range(N):
            t = hbuf[j, rows].astype(F32)
            squares += jnp.sum(t * t, -1, keepdims=True)
        scale = lax.rsqrt(squares * (1.0 / D) + 1e-6)
        for j in range(N):
            bbuf[rows, j * W : (j + 1) * W] = (hbuf[j, rows].astype(F32) * scale * gain_m[:, j * W : (j + 1) * W]).astype(BF16)

    def hidden(c, first, width):
        rows, cols = group_rows(c), pl.ds(first, width)
        b = bbuf[rows, :]
        hid[rows, cols] = (jax.nn.silu(dot(b, wg[:, cols])) * dot(b, wu[:, cols])).astype(BF16)

    def down(c):
        rows = group_rows(c)
        terms(c, 2, rows, hid[rows, :], wd, part2, recv2, down_halves if c == 0 else None)

    with jax.named_scope("k0wait"):
        kcopy(0, 0).wait()
    scores(0, 0, 0)
    kcopy(3, 0).start()
    wbuf[0] = softmax(0)
    with jax.named_scope("k1wait"):
        kcopy(1, 1).wait()
    scores(1, 1, 1)
    kcopy(4, 1).start()
    with jax.named_scope("k2wait"):
        kcopy(2, 2).wait()
    scores(2, 2, 2)

    def mod(g, n):
        return g % n if isinstance(g, int) else lax.rem(g, n)

    def attended(g):
        keep(g, values(mod(g, VS), wbuf.at[mod(g, 2)], 0, U))
        wbuf[mod(g + 1, 2)] = softmax(mod(g + 1, LEAD + 1))

    def arrive(g):
        kcopy(g + LEAD, mod(g + LEAD, NS)).wait()
        vcopy(g, mod(g, VS)).wait()

    def ahead(g):
        scores(g + LEAD, mod(g + LEAD, NS), mod(g + LEAD, LEAD + 1))

    def body(g, _):
        @pl.when(g + LEAD + 2 < G)
        def _():
            kcopy(g + LEAD + 2, mod(g + LEAD + 2, NS)).start()

        vcopy(g + 2, mod(g + 2, VS)).start()
        with jax.named_scope("loopwait"):
            arrive(g)
        attended(g)
        ahead(g)

        @pl.when(g == PARTS[0][1] - 1)
        def _():
            with jax.named_scope("finish0"):
                finish(0)

        @pl.when(g == REDUCE_AT)
        def _():
            with jax.named_scope("reduce1_0"):
                reduce1(0)

        return 0

    with jax.named_scope("loop"):
        lax.fori_loop(0, G - LEAD - 2, body, 0)
    vcopy(G - LEAD, (G - LEAD) % VS).start()
    arrive(G - LEAD - 2)
    attended(G - LEAD - 2)
    @pl.when(here)
    def _():
        with jax.named_scope("finish1"):
            finish(1)

    ahead(G - LEAD - 2)
    vcopy(G - LEAD + 1, (G - LEAD + 1) % VS).start()
    with jax.named_scope("arrive12"):
        arrive(G - LEAD - 1)
    for copy in last:
        copy.start()
    attended(G - LEAD - 1)
    ahead(G - LEAD - 1)
    with jax.named_scope("v13"):
        vcopy(G - LEAD, (G - LEAD) % VS).wait()
    attended(G - LEAD)
    @pl.when(here)
    def _():
        with jax.named_scope("r11"):
            reduce1(1)

    with jax.named_scope("v14"):
        vcopy(G - LEAD + 1, (G - LEAD + 1) % VS).wait()
    attended(G - LEAD + 1)
    for n in range(2):
        loads["wg", n].start()
        loads["wu", n].start()
    for ks in FAR_FIRST:
        for k in ks:
            loads["wd", k].start()
    o = jnp.zeros((16, Q * HEAD), F32)
    for n, copy in enumerate(last):
        with jax.named_scope(f"last{n}"):
            copy.wait()
        o += values((G - 1) % VS, wbuf.at[(G - 1) % 2], n * ULAST, ULAST)
    keep(G - 1, o)
    @pl.when(here)
    def _():
        with jax.named_scope("f2"):
            finish(2)

    with jax.named_scope("n0"):
        norm2(0)
    with jax.named_scope("n01"):
        norm2(1)
    with jax.named_scope("h00"):
        both_halves(0).wait()
        hidden(0, 0 * half, half)
    @pl.when(here)
    def _():
        with jax.named_scope("r12"):
            reduce1(2)

    with jax.named_scope("h01"):
        both_halves(1).wait()
        hidden(0, 1 * half, half)
    @pl.when(here)
    def _():
        with jax.named_scope("d0"):
            down(0)

    @pl.when(here)
    def _():
        with jax.named_scope("n1"):
            norm2(2)

    with jax.named_scope("h1"):
        hidden(1, 0, HID)
    @pl.when(here)
    def _():
        with jax.named_scope("d1"):
            down(1)

    @pl.when(here)
    def _():
        with jax.named_scope("r20"):
            reduce2(0)

    @pl.when(here)
    def _():
        with jax.named_scope("r21"):
            reduce2(1)

    @pl.when(here)
    def _():
        with jax.named_scope("across"):
            some(N // 2 - 1, 0, 3, group_rows(0), ybuf).wait_recv()
            for k in (3, 2, 1):
                across(k).start()


    def put(c):
        rows = group_rows(c)
        for j in range(N):
            out_ref[rows, j * W : (j + 1) * W] = ybuf[j, rows]

    with jax.named_scope("out0"):
        some(N // 2, 2, 0, group_rows(0), ybuf).wait_recv()
    put(0)
    with jax.named_scope("out1"):
        all_seven(1, 3, group_rows(1), ybuf).wait_recv()
    put(1)
    with jax.named_scope("sent"):
        sent = wg.at[pl.ds(0, 4 * (N - 1) * B * W // HID)]
        pltpu.make_async_remote_copy(sent, sent, send_sem, recv_sem.at[0], device_id={"tp": at(1)}, device_id_type=MESH).wait_send()


def solution(mesh):
    any_, vmem = pl.BlockSpec(memory_space=pl.ANY), pl.BlockSpec(memory_space=pltpu.VMEM)

    def step(x, k_cache, v_cache, gain_a, wq, wo, gain_m, w_gate, w_up, w_down):
        return pl.pallas_call(
            layer,
            out_shape=pltpu.VMEM((B, D), BF16),
            in_specs=[any_] * 11,
            out_specs=vmem,
            scratch_shapes=[
                pltpu.VMEM((B, D), BF16),
                pltpu.VMEM((D // 128, 128), BF16),
                pltpu.VMEM((D // 128, 128), BF16),
                pltpu.VMEM((1, D), F32),
                pltpu.VMEM((2, HEAD), F32),
                pltpu.VMEM((NS, Q, U, HEAD), BF16),
                pltpu.VMEM((VS, Q, U, HEAD), BF16),
                pltpu.VMEM((D, QUERIES * HEAD), BF16),
                pltpu.VMEM((QUERIES * HEAD, D), BF16),
                pltpu.VMEM((D, HID), BF16),
                pltpu.VMEM((D, HID), BF16),
                pltpu.VMEM((HID, D), BF16),
                pltpu.VMEM((16 * G, Q * HEAD), BF16),
                pltpu.VMEM((LEAD + 1, 16, U), F32),
                pltpu.VMEM((2, 16, U), BF16),
                pltpu.VMEM((G, Q, QUERIES * HEAD), F32),
                pltpu.VMEM((B, D), BF16),
                pltpu.VMEM((B, HID), BF16),
                pltpu.VMEM((N, B, W), F32),
                *[pltpu.VMEM((N, B, W), BF16)] * 6,
                pltpu.SemaphoreType.DMA((NS,)),
                pltpu.SemaphoreType.DMA((VS,)),
                pltpu.SemaphoreType.DMA((5,)),
                pltpu.SemaphoreType.DMA,
                pltpu.SemaphoreType.DMA((2 * len(PARTS),)),
            ],
            compiler_params=pltpu.CompilerParams(collective_id=0, has_side_effects=True, vmem_limit_bytes=60 * 2**20),
            name="layer",
        )(x, gain_a.reshape(-1, 128), gain_m.reshape(-1, 128), jnp.asarray(rotary_tables()), wq, wo, w_gate, w_up, w_down,
          k_cache.reshape(B, U, HEAD), v_cache.reshape(B, U, HEAD))

    states, cache, columns, rows_of = P("dp", None), P("dp", None, "tp", None), P(None, "tp"), P("tp", None)
    return jax.shard_map(
        step,
        mesh=mesh,
        in_specs=(states, cache, cache, P(None), columns, rows_of, P(None), columns, columns, rows_of),
        out_specs=states,
        check_vma=False,
    )
```
